256 devices in a mesh: seq: 64 (over z, x_hi, y), head: 4 (over x_lo, core).
Axes of the slice: x: 4 (x_hi: 2, x_lo: 2; x = x_hi * 2 + x_lo), y: 4, z: 8, core: 2. Of those that a mesh axis runs over, the one named last changes fastest.
Arguments:
- queries: bfloat16 [16384, 32, 128], P('seq', 'head'), may hold values from -160 to 160
- keys: bfloat16 [16384, 8, 128], P('seq', 'head'), may hold values from -7 to 7
- values: bfloat16 [16384, 8, 128], P('seq', 'head'), may hold values from -6 to 6
- out_weight: bfloat16 [4096, 4096], P('head', 'seq'), may hold values from -0.75 to 0.75
Outputs:
- mixed: bfloat16 [16384, 4096], P('seq', 'head')
The draws below stay inside these ranges and needn't reach their ends.
All inputs are finite; a program needn't handle non-finite values.
Results may differ from the reference program's by a relative error of at most 0.013.
Values may be sent and summed in bfloat16 or wider, within the bound.
A program may use at most 64 MiB of HBM per device.

```python
import jax
import jax.numpy as jnp
from jax import lax

D = 4096
QUERY_HEAD_COUNT = 32
KEY_VALUE_HEADS = 8
HEAD_SIZE = 128
ATTENTION_SPAN = 4096
SEQUENCE_TOKENS = 16384


def key_field(key):
    value_field = jnp.clip(jax.random.normal(jax.random.fold_in(key, 11), (SEQUENCE_TOKENS, KEY_VALUE_HEADS, HEAD_SIZE), jnp.float32), -6.0, 6.0)
    return value_field


def draw_keys(key, part):
    return key_field(key).astype(jnp.bfloat16)


def draw_queries(key, part):
    value_field = 2.0 * jnp.clip(jax.random.normal(jax.random.fold_in(key, 17), (SEQUENCE_TOKENS, QUERY_HEAD_COUNT, HEAD_SIZE), jnp.float32), -6.0, 6.0)
    return value_field.astype(jnp.bfloat16)


def steps_of(key, shape, cuts, smallest, largest):
    gain, own = 1.0, jax.random.fold_in(key, 6)
    for dim, parts in cuts:
        draws = jnp.exp(jax.random.uniform(jax.random.fold_in(own, dim), (parts,), jnp.float32, smallest / len(cuts), largest / len(cuts)))
        gain = gain * jnp.repeat(draws, shape[dim] // parts).reshape([-1 if axis == dim else 1 for axis in range(len(shape))])
    return gain


def noise(stream_key, shape, deviation, most, cuts=(), held_as=jnp.bfloat16):
    drawn = jax.random.normal(stream_key, shape, jnp.float32) * deviation
    if len(cuts) > 0:
        drawn = steps_of(stream_key, shape, cuts, -0.22, 0.18) * drawn
    return jnp.clip(drawn, min=-most, max=most).astype(held_as)


def setup_inputs(seed: int = 0) -> dict:
    arg_keys = jax.random.split(jax.random.key(seed), 5)
    return {
        "queries": draw_queries(jax.random.fold_in(arg_keys[4], 71), 0),
        "keys": draw_keys(jax.random.fold_in(arg_keys[4], 71), 0),
        "values": noise(arg_keys[2], (SEQUENCE_TOKENS, KEY_VALUE_HEADS, HEAD_SIZE), 1.0, 6.0, ((0, 64), (1, 4))),
        "out_weight": noise(arg_keys[3], (QUERY_HEAD_COUNT * HEAD_SIZE, D), (QUERY_HEAD_COUNT * HEAD_SIZE // 64) ** -0.5, 0.75, ((0, 4), (1, 64))),
    }


def reference(queries, keys, values, out_weight):
    rows_per_block = min(512, SEQUENCE_TOKENS)
    query_group_width = QUERY_HEAD_COUNT // KEY_VALUE_HEADS
    score_scale = HEAD_SIZE ** -0.5
    empty_rows = jnp.zeros((ATTENTION_SPAN, KEY_VALUE_HEADS, HEAD_SIZE), keys.dtype)
    padded_keys = jnp.concatenate([empty_rows, keys], 0)
    padded_values = jnp.concatenate([empty_rows, values], 0)

    def attend_block(index):
        offset = (index * rows_per_block).astype(jnp.int32)
        query_tile_rows = lax.dynamic_slice_in_dim(queries, offset, rows_per_block, 0).astype(jnp.float32)
        query_tile_rows = query_tile_rows.reshape(rows_per_block, KEY_VALUE_HEADS, query_group_width, HEAD_SIZE)
        key_block = lax.dynamic_slice_in_dim(padded_keys, offset, ATTENTION_SPAN + rows_per_block, 0).astype(jnp.float32)
        value_block = lax.dynamic_slice_in_dim(padded_values, offset, ATTENTION_SPAN + rows_per_block, 0).astype(jnp.float32)
        query_pos = offset + jnp.arange(rows_per_block, dtype=jnp.int32)
        key_pos = offset - ATTENTION_SPAN + jnp.arange(ATTENTION_SPAN + rows_per_block, dtype=jnp.int32)
        distance = query_pos[:, None] - key_pos[None, :]
        inside = (distance >= 0) & (distance < ATTENTION_SPAN) & (key_pos >= 0)[None, :]
        scores = jnp.einsum("tkgd,skd->kgts", query_tile_rows, key_block) * score_scale
        scores = jnp.where(inside, scores, -1e30)
        highest = jnp.max(scores, axis=-1, keepdims=True)
        weights = jnp.where(inside, jnp.exp(scores - highest), 0.0)
        denominator = jnp.sum(weights, axis=-1)
        probs = weights.astype(jnp.bfloat16).astype(jnp.float32)
        numerator = jnp.einsum("kgts,skd->kgtd", probs, value_block)
        result = numerator / denominator[..., None]
        return jnp.transpose(result, (2, 0, 1, 3)).reshape(rows_per_block, QUERY_HEAD_COUNT * HEAD_SIZE).astype(jnp.bfloat16)

    attended = lax.map(attend_block, jnp.arange(SEQUENCE_TOKENS // rows_per_block, dtype=jnp.int32))
    attended = attended.reshape(SEQUENCE_TOKENS, QUERY_HEAD_COUNT * HEAD_SIZE)
    return jnp.dot(attended, out_weight, preferred_element_type=jnp.float32).astype(jnp.bfloat16)
```

```python
import functools

import jax
import jax.numpy as jnp
from jax import lax
from jax.experimental import pallas as pl
from jax.experimental.pallas import tpu as pltpu
from jax.sharding import PartitionSpec as P

MESH = pl.DeviceIdType.MESH
NT = (((1,), (1,)), ((), ()))
BIG = 1e30
LOG2E = 1.4426950408889634
HS = 128
SH = 256
CH = 512
ROWS = 128
BF = jnp.bfloat16
F32 = jnp.float32


def kernel(
    q_in,
    kv_in,
    w_in,
    out,
    qb,
    own,
    oth,
    wb,
    mx,
    acc,
    ab,
    pf,
    pa,
    pr,
    rb,
    ss_kv, rs_kv, ss_q, rs_q,
    ss_z, rs_z, ss_x, rs_x,
    ss_c, rs_c,
    ss_w, rs_w,
    ss_wc, rs_wc,
    ss_a, rs_a,
    ss_p, rs_p,
    ss_o, rs_o,
):
    seq = lax.axis_index("seq")
    head = lax.axis_index("head")
    z, xh, y = seq // 8, (seq // 4) % 2, seq % 4
    xl, c = head // 2, head % 2

    def dev(zz, xx, yy, ll, cc):
        return (zz * 8 + xx * 4 + yy, ll * 2 + cc)

    zp, zm = lax.rem(z + 1, 8), lax.rem(z + 7, 8)
    d_zp = dev(zp, xh, y, xl, c)
    d_zm = dev(zm, xh, y, xl, c)
    d_x = dev(z, 1 - xh, y, xl, c)
    d_c = dev(z, xh, y, xl, 1 - c)
    d_l = dev(z, xh, y, 1 - xl, c)

    def remote(src, dst, ss, rs, device):
        return pltpu.make_async_remote_copy(
            src_ref=src, dst_ref=dst, send_sem=ss, recv_sem=rs,
            device_id=device, device_id_type=MESH,
        )

    barrier = pltpu.get_barrier_semaphore()
    for dy in range(4):
        for dc in range(2):
            if dy or dc:
                pl.semaphore_signal(
                    barrier, inc=1, device_id_type=MESH,
                    device_id=dev(z, xh, lax.rem(y + dy, 4), xl, lax.rem(c + dc, 2)),
                )
    for d in (d_zp, d_zm, d_x, d_l):
        pl.semaphore_signal(barrier, inc=1, device_id=d, device_id_type=MESH)
    pl.semaphore_wait(barrier, 11)

    jy = y % 2

    def to_head(i):
        dest = dev(z, xh, 2 * c + i, xl, y // 2)
        kv = remote(kv_in.at[i], own.at[0, :, pl.ds(jy * SH, SH), :], ss_kv.at[i], rs_kv.at[jy], dest)
        q = remote(q_in.at[i], qb.at[jy], ss_q.at[i], rs_q.at[jy], dest)
        return kv, q

    mine_here = c == y // 2

    def is_remote(i):
        return jnp.logical_not(jnp.logical_and(mine_here, jy == i))

    for i in range(2):
        @pl.when(is_remote(i))
        def _():
            to_head(i)[0].start()

    w_x = remote(w_in, wb.at[c, z, xh], ss_w.at[0], rs_w.at[0], d_x)
    w_x.start()
    for i in range(2):
        @pl.when(is_remote(i))
        def _():
            to_head(i)[1].start()

        @pl.when(jnp.logical_not(is_remote(i)))
        def _():
            own[0, :, i * SH : (i + 1) * SH, :] = kv_in[i]
            qb[i] = q_in[i]

    wb[c, z, xh] = w_in[...]

    def wait_in(which):
        for j in range(2):
            @pl.when(jnp.logical_not(jnp.logical_and(mine_here, jy == j)))
            def _():
                if which == 0:
                    remote(kv_in.at[0], own.at[0, :, pl.ds(j * SH, SH), :], ss_kv.at[0], rs_kv.at[j], d_c).wait_recv()
                else:
                    remote(q_in.at[0], qb.at[j], ss_q.at[0], rs_q.at[j], d_c).wait_recv()

    def w_up(s):
        b = wb.at[c, lax.rem(z + 8 - s, 8)]
        return remote(b, b, ss_w.at[1 + s], rs_w.at[1 + s], d_zp)

    def w_down(s):
        b = wb.at[c, lax.rem(z + s, 8)]
        return remote(b, b, ss_w.at[4 + s], rs_w.at[4 + s], d_zm)

    def w_core(k, block):
        b = wb.at[c, block]
        return remote(b, b, ss_wc.at[k], rs_wc.at[k], d_c)

    def w_up_got(s):
        w_up(s).wait_recv()
        if s < 2:
            w_up(s + 1).start()
        w_core(1 + s, lax.rem(z + 7 - s, 8)).start()

    def w_down_got(s):
        w_down(s).wait_recv()
        if s < 3:
            w_down(s + 1).start()
        w_core(4 + s, lax.rem(z + 1 + s, 8)).start()

    z_send = [
        remote(own.at[0], own.at[2], ss_z.at[0], rs_z.at[0], d_zp),
        remote(own.at[2], own.at[4], ss_z.at[1], rs_z.at[1], d_zp),
    ]

    def x_send(item, k):
        return remote(own.at[item], own.at[1 + 2 * k], ss_x.at[k], rs_x.at[k], d_x)

    def c_send(item, k):
        return remote(own.at[item], oth.at[k], ss_c.at[k], rs_c.at[k], d_c)

    wait_in(0)
    z_send[0].start()

    @pl.when(xh == 0)
    def _():
        x_send(0, 0).start()

    @pl.when(c == 0)
    def _():
        c_send(0, 0).start()

    w_x.wait_recv()
    w_core(0, z).start()
    w_up(0).start()
    w_down(0).start()
    wait_in(1)

    hg = 4 * z + 2 * xh + c
    scale = LOG2E / HS**0.5

    def bias(delta):
        return jnp.where(hg >= delta, 0.0, BIG).astype(F32)

    ones = jnp.ones((CH, HS), BF)

    def attend(j, segs, first=False):
        for g in range(4):
            for h in range(SH // ROWS):
                rows = slice(h * ROWS, (h + 1) * ROWS)
                q = qb[j, g, rows, :]
                scores, tops = [], []
                for ref, lo, size, mask, b in segs:
                    s = lax.dot_general(q, ref[0, lo : lo + size, :], NT, preferred_element_type=F32)
                    if mask is not None:
                        t = lax.broadcasted_iota(jnp.int32, s.shape, 0) + h * ROWS
                        k = lax.broadcasted_iota(jnp.int32, s.shape, 1)
                        s = jnp.where(k <= t if mask == "upto" else k > t, s, -BIG)
                    m = jnp.max(s, axis=1, keepdims=True)
                    scores.append(s)
                    tops.append(m if b is None else m - b)
                top = tops[0]
                for m in tops[1:]:
                    top = jnp.maximum(top, m)
                if first:
                    new = jnp.broadcast_to(top, (ROWS, HS))
                else:
                    old = mx[j, g, rows, :]
                    new = jnp.maximum(old, top)
                total = None
                for s, (ref, lo, size, mask, b) in zip(scores, segs):
                    m = new[:, :1] if b is None else new[:, :1] + b
                    p = jnp.exp2((s - m) * scale).astype(BF)
                    v = jnp.concatenate([ref[1, lo : lo + size, :], ones[:size]], 1)
                    u = jnp.dot(p, v, preferred_element_type=F32)
                    total = u if total is None else total + u
                if first:
                    acc[j, g, rows, :] = total
                else:
                    a = jnp.exp2((old - new) * scale)
                    acc[j, g, rows, :] = acc[j, g, rows, :] * jnp.concatenate([a, a], 1) + total
                mx[j, g, rows, :] = new

    def diagonal(j):
        last = (own.at[0], j * SH, SH, "upto", None)
        return [(own.at[0], 0, SH, None, None), last] if j else [last]

    def far(j):
        edge = (own.at[4], j * SH, SH, "after", bias(8))
        return [edge] if j else [edge, (own.at[4], SH, SH, None, bias(8))]

    def full(ref, delta):
        return (ref, 0, CH, None, bias(delta))

    odd = [jnp.where(c == 0, p, q) for p, q in ((3, 1), (1, 5), (7, 3), (5, 7))]

    z_send[0].wait_recv()
    z_send[1].start()

    @pl.when(xh == 0)
    def _():
        x_send(2, 1).start()

    @pl.when(xh == 1)
    def _():
        x_send(2, 0).start()

    @pl.when(c == 0)
    def _():
        c_send(2, 1).start()

    @pl.when(c == 1)
    def _():
        c_send(2, 0).start()

    for j in range(2):
        attend(j, diagonal(j) + [full(own.at[2], 4)], first=True)
    w_up_got(0)
    w_down_got(0)

    x_send(0, 0).wait_recv()

    @pl.when(c == 0)
    def _():
        c_send(1, 2).start()

    @pl.when(c == 1)
    def _():
        c_send(1, 1).start()

    c_send(0, 0).wait_recv()
    for j in range(2):
        attend(j, [full(own.at[1], 2), full(oth.at[0], odd[0])])

    z_send[1].wait_recv()

    @pl.when(xh == 1)
    def _():
        x_send(4, 1).start()

    @pl.when(c == 1)
    def _():
        c_send(4, 2).start()

    w_up_got(1)
    w_down_got(1)
    c_send(0, 1).wait_recv()
    c_send(0, 2).wait_recv()

    attend(0, far(0) + [full(oth.at[1], odd[1]), full(oth.at[2], odd[2])])

    x_send(0, 1).wait_recv()
    c_send(3, 3).start()
    c_send(0, 3).wait_recv()
    w_up_got(2)
    w_down_got(2)

    def a_send(j, k):
        b = ab.at[y, j]
        return remote(b, b, ss_a.at[k, j], rs_a.at[k, j], dev(z, xh, lax.rem(y + k + 1, 4), xl, c))

    def finish(j):
        attend(j, [full(own.at[3], 6), full(oth.at[3], odd[3])])
        for g in range(4):
            a = acc[j, g]
            ab[y, j, :, g * HS : (g + 1) * HS] = (a[:, :HS] / a[:, HS:]).astype(BF)
        for k in range(3):
            a_send(j, k).start()

    finish(0)
    attend(1, far(1) + [full(oth.at[1], odd[1]), full(oth.at[2], odd[2])])
    finish(1)
    w_down_got(3)
    for k in range(8):
        w_core(k, z).wait_recv()

    def partial(j, half, i):
        total = None
        zz = half * 4 + i * 2
        for yy in range(4):
            w = wb[yy // 2, pl.ds(zz, 2), :, :, (yy % 2) * CH : (yy % 2 + 1) * CH].reshape(SH, CH)
            u = lax.dot_general(ab[yy, j], w, NT, preferred_element_type=F32)
            total = u if total is None else total + u
        return total

    def p_send(j, i):
        return remote(pa.at[j, i], pr.at[j, i], ss_p.at[j, i], rs_p.at[j, i], d_l)

    def o_send(j, i):
        return remote(rb.at[j, i], out.at[y], ss_o.at[j, i], rs_o.at[y], dev(z, xh, 2 * c + j, xl, i))

    def o_here(j, i):
        return jnp.logical_and(y == 2 * c + j, c == i)

    for j in range(2):
        for k in range(3):
            a_send(j, k).wait_recv()
        for i in range(2):
            pa[j, i] = partial(j, 1 - xl, i).astype(BF)
            p_send(j, i).start()
        for i in range(2):
            pf[j, i] = partial(j, xl, i)
    for j in range(2):
        for i in range(2):
            p_send(j, i).wait_recv()
            total = (pf[j, i] + pr[j, i].astype(F32)).astype(BF)

            @pl.when(o_here(j, i))
            def _():
                out[y] = total

            @pl.when(jnp.logical_not(o_here(j, i)))
            def _():
                rb[j, i] = total
                o_send(j, i).start()

    for yy in range(4):
        @pl.when(jnp.logical_not(jnp.logical_and(yy == y, c == y // 2)))
        def _():
            remote(rb.at[0, 0], out.at[yy], ss_o.at[0, 0], rs_o.at[yy], d_c).wait_recv()
    for i in range(2):
        @pl.when(is_remote(i))
        def _():
            for copy in to_head(i):
                copy.wait_send()
    w_x.wait_send()
    for s in range(3):
        w_up(s).wait_send()
    for s in range(4):
        w_down(s).wait_send()
    for k in range(8):
        w_core(k, z).wait_send()
    for k in range(2):
        z_send[k].wait_send()
        x_send(0, k).wait_send()
    for k in range(4):
        c_send(0, k).wait_send()
    for j in range(2):
        for k in range(3):
            a_send(j, k).wait_send()
        for i in range(2):
            p_send(j, i).wait_send()

            @pl.when(jnp.logical_not(o_here(j, i)))
            def _():
                o_send(j, i).wait_send()


def body(queries, keys, values, out_weight):
    tokens = queries.shape[0]
    q = queries.reshape(tokens, 2, 4, HS).transpose(1, 2, 0, 3)
    kv = jnp.stack([keys, values]).transpose(2, 0, 1, 3)
    dma = pltpu.SemaphoreType.DMA
    sems = [dma((2,))] * 8 + [dma((4,))] * 2 + [dma((8,))] * 4 + [dma((3, 2))] * 2 + [dma((2, 2))] * 3 + [dma((4,))]
    vmem = pl.BlockSpec(memory_space=pltpu.VMEM)
    r = pl.pallas_call(
        kernel,
        name="layer",
        out_shape=jax.ShapeDtypeStruct((4, SH, SH), BF),
        in_specs=[vmem] * 3,
        out_specs=vmem,
        scratch_shapes=[
            pltpu.VMEM((2, 4, SH, HS), BF),
            pltpu.VMEM((5, 2, CH, HS), BF),
            pltpu.VMEM((4, 2, CH, HS), BF),
            pltpu.VMEM((2, 8, 2, 64, 1024), BF),
            pltpu.VMEM((2, 4, SH, HS), F32),
            pltpu.VMEM((2, 4, SH, 2 * HS), F32),
            pltpu.VMEM((4, 2, SH, CH), BF),
            pltpu.VMEM((2, 2, SH, SH), F32),
            pltpu.VMEM((2, 2, SH, SH), BF),
            pltpu.VMEM((2, 2, SH, SH), BF),
            pltpu.VMEM((2, 2, SH, SH), BF),
            *sems,
        ],
        compiler_params=pltpu.CompilerParams(
            collective_id=0, has_side_effects=True, vmem_limit_bytes=48 * 2**20
        ),
    )(q, kv, out_weight.T)
    return r.reshape(4, tokens, 4, 64).transpose(1, 2, 0, 3).reshape(tokens, 1024)


def solution(mesh):
    return jax.shard_map(
        body,
        mesh=mesh,
        in_specs=(
            P("seq", "head", None),
            P("seq", "head", None),
            P("seq", "head", None),
            P("head", "seq"),
        ),
        out_specs=P("seq", "head"),
        check_vma=False,
    )
```

```python
import functools

import jax
import jax.numpy as jnp
from jax import lax
from jax.experimental import pallas as pl
from jax.experimental.pallas import tpu as pltpu
from jax.sharding import PartitionSpec as P

MESH = pl.DeviceIdType.MESH
NT = (((1,), (1,)), ((), ()))
BIG = 1e30
LOG2E = 1.4426950408889634
HS = 128
SH = 256
CH = 512
ROWS = 128
DOWN, UP = 5, 2
BF = jnp.bfloat16
F32 = jnp.float32


def kernel(
    q_in,
    kv_in,
    w_in,
    out,
    qb,
    own,
    oth,
    wb,
    mx,
    acc,
    ab,
    pf,
    pa,
    pr,
    rb,
    ss_kv, rs_kv, ss_q, rs_q,
    ss_z, rs_z, ss_x, rs_x,
    ss_c, rs_c,
    ss_wx, rs_wx,
    ss_w, rs_w,
    ss_wc, rs_wc,
    ss_a, rs_a,
    ss_r, rs_r,
    ss_p, rs_p,
    ss_o, rs_o,
):
    seq = lax.axis_index("seq")
    head = lax.axis_index("head")
    z, xh, y = seq // 8, (seq // 4) % 2, seq % 4
    xl, c = head // 2, head % 2

    def dev(zz, xx, yy, ll, cc):
        return (zz * 8 + xx * 4 + yy, ll * 2 + cc)

    zp, zm = lax.rem(z + 1, 8), lax.rem(z + 7, 8)
    d_zp = dev(zp, xh, y, xl, c)
    d_zm = dev(zm, xh, y, xl, c)
    d_x = dev(z, 1 - xh, y, xl, c)
    d_c = dev(z, xh, y, xl, 1 - c)
    d_l = dev(z, xh, y, 1 - xl, c)

    def remote(src, dst, ss, rs, device):
        return pltpu.make_async_remote_copy(
            src_ref=src, dst_ref=dst, send_sem=ss, recv_sem=rs,
            device_id=device, device_id_type=MESH,
        )

    barrier = pltpu.get_barrier_semaphore()
    for dy in range(4):
        for dc in range(2):
            if dy or dc:
                pl.semaphore_signal(
                    barrier, inc=1, device_id_type=MESH,
                    device_id=dev(z, xh, lax.rem(y + dy, 4), xl, lax.rem(c + dc, 2)),
                )
    for d in (d_zp, d_zm, d_x, d_l):
        pl.semaphore_signal(barrier, inc=1, device_id=d, device_id_type=MESH)
    pl.semaphore_wait(barrier, 11)

    jy = y % 2

    def to_head(i):
        dest = dev(z, xh, 2 * c + i, xl, y // 2)
        kv = remote(kv_in.at[i], own.at[0, :, pl.ds(jy * SH, SH), :], ss_kv.at[i], rs_kv.at[jy], dest)
        q = remote(q_in.at[i], qb.at[jy], ss_q.at[i], rs_q.at[jy], dest)
        return kv, q

    mine_here = c == y // 2

    def is_remote(i):
        return jnp.logical_not(jnp.logical_and(mine_here, jy == i))

    for i in range(2):
        @pl.when(is_remote(i))
        def _():
            to_head(i)[0].start()

    w_x = remote(w_in, wb.at[c, z, xh], ss_wx.at[0], rs_wx.at[0], d_x)
    w_x.start()
    for i in range(2):
        @pl.when(is_remote(i))
        def _():
            to_head(i)[1].start()

        @pl.when(jnp.logical_not(is_remote(i)))
        def _():
            own[0, :, i * SH : (i + 1) * SH, :] = kv_in[i]
            qb[i] = q_in[i]

    wb[c, z, xh] = w_in[...]

    def wait_in(which, j):
        @pl.when(jnp.logical_not(jnp.logical_and(mine_here, jy == j)))
        def _():
            if which == 0:
                remote(kv_in.at[0], half(0, j), ss_kv.at[0], rs_kv.at[j], d_c).wait_recv()
            else:
                remote(q_in.at[0], qb.at[j], ss_q.at[0], rs_q.at[j], d_c).wait_recv()

    def w_ring(k, s, h):
        b = wb.at[c, lax.rem(z + s, 8) if k == 0 else lax.rem(z + 8 - s, 8), h]
        n = s if k == 0 else DOWN + s
        return remote(b, b, ss_w.at[n, h], rs_w.at[n, h], d_zp if k else d_zm)

    def w_core(n, block):
        b = wb.at[c, block]
        return remote(b, b, ss_wc.at[n], rs_wc.at[n], d_c)

    def w_got(k, s):
        for h in range(2):
            w_ring(k, s, h).wait_recv()
            if s + 1 < (UP if k else DOWN):
                w_ring(k, s + 1, h).start()
        if k == 0:
            w_core(1 + s, lax.rem(z + 1 + s, 8)).start()
        else:
            w_core(1 + DOWN + s, lax.rem(z + 7 - s, 8)).start()

    def half(item, h):
        return own.at[item, :, pl.ds(h * SH, SH), :]

    def z_send(k, h):
        return remote(half(2 * k, h), half(2 * k + 2, h), ss_z.at[k, h], rs_z.at[k, h], d_zp)

    def x_send(item, k, h):
        return remote(half(item, h), half(1 + 2 * k, h), ss_x.at[k, h], rs_x.at[k, h], d_x)

    def c_send(item, k, h):
        return remote(half(item, h), oth.at[k, :, pl.ds(h * SH, SH), :], ss_c.at[k, h], rs_c.at[k, h], d_c)

    def start_if(condition, make, *args):
        @pl.when(condition)
        def _():
            make(*args).start()

    for h in range(2):
        wait_in(0, h)
        z_send(0, h).start()
        start_if(xh == 0, x_send, 0, 0, h)
        start_if(c == 0, c_send, 0, 0, h)
    w_x.wait_recv()
    for h in range(2):
        w_ring(0, 0, h).start()
    w_core(0, z).start()
    for j in range(2):
        wait_in(1, j)

    def got_z1(h):
        z_send(0, h).wait_recv()
        z_send(1, h).start()
        start_if(xh == 0, x_send, 2, 1, h)
        start_if(xh == 1, x_send, 2, 0, h)
        start_if(c == 0, c_send, 2, 1, h)
        start_if(c == 1, c_send, 2, 0, h)

    def got_a(h):
        x_send(0, 0, h).wait_recv()
        start_if(c == 0, c_send, 1, 2, h)
        start_if(c == 1, c_send, 1, 1, h)

    def got_z2(h):
        z_send(1, h).wait_recv()
        start_if(xh == 1, x_send, 4, 1, h)
        start_if(c == 1, c_send, 4, 2, h)

    def got_b(h):
        x_send(0, 1, h).wait_recv()
        c_send(3, 3, h).start()

    def got_c(k):
        for h in range(2):
            c_send(0, k, h).wait_recv()

    hg = 4 * z + 2 * xh + c
    scale = LOG2E / HS**0.5

    def bias(delta):
        return jnp.where(hg >= delta, 0.0, BIG).astype(F32)

    ones = jnp.ones((CH, HS), BF)

    def attend(j, segs, first=False):
        for g in range(4):
            for h in range(SH // ROWS):
                rows = slice(h * ROWS, (h + 1) * ROWS)
                q = qb[j, g, rows, :]
                scores, tops = [], []
                for ref, lo, size, mask, b in segs:
                    s = lax.dot_general(q, ref[0, lo : lo + size, :], NT, preferred_element_type=F32)
                    if mask is not None:
                        t = lax.broadcasted_iota(jnp.int32, s.shape, 0) + h * ROWS
                        k = lax.broadcasted_iota(jnp.int32, s.shape, 1)
                        s = jnp.where(k <= t if mask == "upto" else k > t, s, -BIG)
                    m = jnp.max(s, axis=1, keepdims=True)
                    scores.append(s)
                    tops.append(m if b is None else m - b)
                top = tops[0]
                for m in tops[1:]:
                    top = jnp.maximum(top, m)
                if first:
                    new = jnp.broadcast_to(top, (ROWS, HS))
                else:
                    old = mx[j, g, rows, :]
                    new = jnp.maximum(old, top)
                total = None
                for s, (ref, lo, size, mask, b) in zip(scores, segs):
                    m = new[:, :1] if b is None else new[:, :1] + b
                    p = jnp.exp2((s - m) * scale).astype(BF)
                    v = jnp.concatenate([ref[1, lo : lo + size, :], ones[:size]], 1)
                    u = jnp.dot(p, v, preferred_element_type=F32)
                    total = u if total is None else total + u
                if first:
                    acc[j, g, rows, :] = total
                else:
                    a = jnp.exp2((old - new) * scale)
                    acc[j, g, rows, :] = acc[j, g, rows, :] * jnp.concatenate([a, a], 1) + total
                mx[j, g, rows, :] = new

    def diagonal(j):
        last = (own.at[0], j * SH, SH, "upto", None)
        return [(own.at[0], 0, SH, None, None), last] if j else [last]

    def far(j):
        edge = (own.at[4], j * SH, SH, "after", bias(8))
        return [edge] if j else [edge, (own.at[4], SH, SH, None, bias(8))]

    def full(ref, delta):
        return (ref, 0, CH, None, bias(delta))

    odd = [jnp.where(c == 0, p, q) for p, q in ((3, 1), (1, 5), (7, 3), (5, 7))]

    yp, ym = lax.rem(y + 1, 4), lax.rem(y + 3, 4)

    def a_send(k, j):
        b = ab.at[y, j]
        return remote(b, b, ss_a.at[k, j], rs_a.at[k, j], dev(z, xh, ym if k else yp, xl, c))

    def a_relay(k, j):
        b = ab.at[yp if k else ym, j, pl.ds(k * ROWS, ROWS), :]
        return remote(b, b, ss_r.at[k, j], rs_r.at[k, j], dev(z, xh, ym if k else yp, xl, c))

    def a_got(j):
        for k in range(2):
            a_send(k, j).wait_recv()
            a_relay(k, j).start()

    def finish(j):
        attend(j, [full(own.at[3], 6), full(oth.at[3], odd[3])])
        for g in range(4):
            a = acc[j, g]
            ab[y, j, :, g * HS : (g + 1) * HS] = (a[:, :HS] / a[:, HS:]).astype(BF)
        for k in range(2):
            a_send(k, j).start()

    got_z1(0)
    got_z1(1)
    for h in range(2):
        w_ring(1, 0, h).start()
    attend(0, diagonal(0) + [full(own.at[2], 4)], first=True)
    w_got(0, 0)
    attend(1, diagonal(1) + [full(own.at[2], 4)], first=True)
    got_a(0)
    got_z2(0)
    got_c(0)
    for j in range(2):
        attend(j, [full(oth.at[0], odd[0])])
    got_a(1)
    got_z2(1)
    attend(0, [full(own.at[1], 2)] + far(0))
    got_b(0)
    got_c(1)
    got_c(2)
    attend(0, [full(oth.at[1], odd[1]), full(oth.at[2], odd[2])])
    w_got(0, 1)
    got_b(1)
    attend(1, [full(own.at[1], 2)] + far(1))
    got_c(3)
    finish(0)
    attend(1, [full(oth.at[1], odd[1]), full(oth.at[2], odd[2])])
    finish(1)
    w_got(1, 0)
    w_got(0, 2)
    a_got(0)
    w_got(1, 1)
    w_got(0, 3)
    a_got(1)
    w_got(0, 4)
    for k in range(8):
        w_core(k, z).wait_recv()

    def partial(j, half, i):
        total = None
        zz = half * 4 + i * 2
        for yy in range(4):
            w = wb[yy // 2, pl.ds(zz, 2), :, :, (yy % 2) * CH : (yy % 2 + 1) * CH].reshape(SH, CH)
            u = lax.dot_general(ab[yy, j], w, NT, preferred_element_type=F32)
            total = u if total is None else total + u
        return total

    def p_send(j, i):
        return remote(pa.at[j, i], pr.at[j, i], ss_p.at[j, i], rs_p.at[j, i], d_l)

    def o_send(j, i):
        return remote(rb.at[j, i], out.at[y], ss_o.at[j, i], rs_o.at[y], dev(z, xh, 2 * c + j, xl, i))

    def o_here(j, i):
        return jnp.logical_and(y == 2 * c + j, c == i)

    for j in range(2):
        for k in range(2):
            a_relay(k, j).wait_recv()
        for i in range(2):
            pa[j, i] = partial(j, 1 - xl, i).astype(BF)
            p_send(j, i).start()
        for i in range(2):
            pf[j, i] = partial(j, xl, i)
    for j in range(2):
        for i in range(2):
            p_send(j, i).wait_recv()
            total = (pf[j, i] + pr[j, i].astype(F32)).astype(BF)

            @pl.when(o_here(j, i))
            def _():
                out[y] = total

            @pl.when(jnp.logical_not(o_here(j, i)))
            def _():
                rb[j, i] = total
                o_send(j, i).start()

    for yy in range(4):
        @pl.when(jnp.logical_not(jnp.logical_and(yy == y, c == y // 2)))
        def _():
            remote(rb.at[0, 0], out.at[yy], ss_o.at[0, 0], rs_o.at[yy], d_c).wait_recv()
    for i in range(2):
        @pl.when(is_remote(i))
        def _():
            for copy in to_head(i):
                copy.wait_send()
    w_x.wait_send()
    for h in range(2):
        for k in range(2):
            for n in range(UP if k else DOWN):
                w_ring(k, n, h).wait_send()
            z_send(k, h).wait_send()
            x_send(0, k, h).wait_send()
        for k in range(4):
            c_send(0, k, h).wait_send()
    for k in range(8):
        w_core(k, z).wait_send()
    for j in range(2):
        for k in range(2):
            a_send(k, j).wait_send()
            a_relay(k, j).wait_send()
        for i in range(2):
            p_send(j, i).wait_send()

            @pl.when(jnp.logical_not(o_here(j, i)))
            def _():
                o_send(j, i).wait_send()


def body(queries, keys, values, out_weight):
    tokens = queries.shape[0]
    q = queries.reshape(tokens, 2, 4, HS).transpose(1, 2, 0, 3)
    kv = jnp.stack([keys, values]).transpose(2, 0, 1, 3)
    dma = pltpu.SemaphoreType.DMA
    shapes = [(2,)] * 4 + [(2, 2)] * 4 + [(4, 2)] * 2 + [(1,)] * 2 + [(DOWN + UP, 2)] * 2 + [(8,)] * 2 + [(2, 2)] * 7 + [(4,)]
    sems = [dma(shape) for shape in shapes]
    vmem = pl.BlockSpec(memory_space=pltpu.VMEM)
    r = pl.pallas_call(
        kernel,
        name="layer",
        out_shape=jax.ShapeDtypeStruct((4, SH, SH), BF),
        in_specs=[vmem] * 3,
        out_specs=vmem,
        scratch_shapes=[
            pltpu.VMEM((2, 4, SH, HS), BF),
            pltpu.VMEM((5, 2, CH, HS), BF),
            pltpu.VMEM((4, 2, CH, HS), BF),
            pltpu.VMEM((2, 8, 2, 64, 1024), BF),
            pltpu.VMEM((2, 4, SH, HS), F32),
            pltpu.VMEM((2, 4, SH, 2 * HS), F32),
            pltpu.VMEM((4, 2, SH, CH), BF),
            pltpu.VMEM((2, 2, SH, SH), F32),
            pltpu.VMEM((2, 2, SH, SH), BF),
            pltpu.VMEM((2, 2, SH, SH), BF),
            pltpu.VMEM((2, 2, SH, SH), BF),
            *sems,
        ],
        compiler_params=pltpu.CompilerParams(
            collective_id=0, has_side_effects=True, vmem_limit_bytes=48 * 2**20
        ),
    )(q, kv, out_weight.T)
    return r.reshape(4, tokens, 4, 64).transpose(1, 2, 0, 3).reshape(tokens, 1024)


def solution(mesh):
    return jax.shard_map(
        body,
        mesh=mesh,
        in_specs=(
            P("seq", "head", None),
            P("seq", "head", None),
            P("seq", "head", None),
            P("head", "seq"),
        ),
        out_specs=P("seq", "head"),
        check_vma=False,
    )
```

```python
import functools

import jax
import jax.numpy as jnp
from jax import lax
from jax.experimental import pallas as pl
from jax.experimental.pallas import tpu as pltpu
from jax.sharding import PartitionSpec as P

MESH = pl.DeviceIdType.MESH
NT = (((1,), (1,)), ((), ()))
BIG = 1e30
LOG2E = 1.4426950408889634
HS = 128
SH = 256
CH = 512
ROWS = 128
DOWN, UP = 5, 2
BF = jnp.bfloat16
F32 = jnp.float32


def kernel(
    q_in,
    kv_in,
    w_in,
    out,
    qb,
    own,
    oth,
    wb,
    mx,
    acc,
    ab,
    pf,
    pa,
    pr,
    rb,
    ss_kv, rs_kv, ss_q, rs_q,
    ss_z, rs_z, ss_x, rs_x,
    ss_c, rs_c,
    ss_wx, rs_wx,
    ss_w, rs_w,
    ss_wc, rs_wc,
    ss_a, rs_a,
    ss_r, rs_r,
    ss_p, rs_p,
    ss_o, rs_o,
):
    seq = lax.axis_index("seq")
    head = lax.axis_index("head")
    z, xh, y = seq // 8, (seq // 4) % 2, seq % 4
    xl, c = head // 2, head % 2

    def dev(zz, xx, yy, ll, cc):
        return (zz * 8 + xx * 4 + yy, ll * 2 + cc)

    zp, zm = lax.rem(z + 1, 8), lax.rem(z + 7, 8)
    d_zp = dev(zp, xh, y, xl, c)
    d_zm = dev(zm, xh, y, xl, c)
    d_x = dev(z, 1 - xh, y, xl, c)
    d_c = dev(z, xh, y, xl, 1 - c)
    d_l = dev(z, xh, y, 1 - xl, c)

    def remote(src, dst, ss, rs, device):
        return pltpu.make_async_remote_copy(
            src_ref=src, dst_ref=dst, send_sem=ss, recv_sem=rs,
            device_id=device, device_id_type=MESH,
        )

    barrier = pltpu.get_barrier_semaphore()
    for dy in range(4):
        for dc in range(2):
            if dy or dc:
                pl.semaphore_signal(
                    barrier, inc=1, device_id_type=MESH,
                    device_id=dev(z, xh, lax.rem(y + dy, 4), xl, lax.rem(c + dc, 2)),
                )
    for d in (d_zp, d_zm, d_x, d_l):
        pl.semaphore_signal(barrier, inc=1, device_id=d, device_id_type=MESH)
    pl.semaphore_wait(barrier, 11)

    jy = y % 2

    def to_head(i):
        dest = dev(z, xh, 2 * c + i, xl, y // 2)
        kv = remote(kv_in.at[i], own.at[0, :, pl.ds(jy * SH, SH), :], ss_kv.at[i], rs_kv.at[jy], dest)
        q = remote(q_in.at[i], qb.at[jy], ss_q.at[i], rs_q.at[jy], dest)
        return kv, q

    mine_here = c == y // 2

    def is_remote(i):
        return jnp.logical_not(jnp.logical_and(mine_here, jy == i))

    for i in range(2):
        @pl.when(is_remote(i))
        def _():
            to_head(i)[0].start()

    w_x = remote(w_in, wb.at[c, z, xh], ss_wx.at[0], rs_wx.at[0], d_x)
    w_x.start()
    for i in range(2):
        @pl.when(is_remote(i))
        def _():
            to_head(i)[1].start()

        @pl.when(jnp.logical_not(is_remote(i)))
        def _():
            own[0, :, i * SH : (i + 1) * SH, :] = kv_in[i]
            qb[i] = q_in[i]

    wb[c, z, xh] = w_in[...]

    def wait_in(which, j):
        @pl.when(jnp.logical_not(jnp.logical_and(mine_here, jy == j)))
        def _():
            if which == 0:
                remote(kv_in.at[0], half(0, j), ss_kv.at[0], rs_kv.at[j], d_c).wait_recv()
            else:
                remote(q_in.at[0], qb.at[j], ss_q.at[0], rs_q.at[j], d_c).wait_recv()

    def w_ring(k, s, h):
        b = wb.at[c, lax.rem(z + s, 8) if k == 0 else lax.rem(z + 8 - s, 8), h]
        n = s if k == 0 else DOWN + s
        return remote(b, b, ss_w.at[n, h], rs_w.at[n, h], d_zp if k else d_zm)

    def w_core(n, block):
        b = wb.at[c, block]
        return remote(b, b, ss_wc.at[n], rs_wc.at[n], d_c)

    def w_got(k, s, h):
        w_ring(k, s, h).wait_recv()
        if s + 1 < (UP if k else DOWN):
            w_ring(k, s + 1, h).start()
        if h == 1 and k == 0:
            w_core(1 + s, lax.rem(z + 1 + s, 8)).start()
        if h == 1 and k == 1:
            w_core(1 + DOWN + s, lax.rem(z + 7 - s, 8)).start()

    def half(item, h):
        return own.at[item, :, pl.ds(h * SH, SH), :]

    def z_send(k, h):
        return remote(half(2 * k, h), half(2 * k + 2, h), ss_z.at[k, h], rs_z.at[k, h], d_zp)

    def x_send(item, k, h):
        return remote(half(item, h), half(1 + 2 * k, h), ss_x.at[k, h], rs_x.at[k, h], d_x)

    def c_send(item, k, h):
        return remote(half(item, h), oth.at[k, :, pl.ds(h * SH, SH), :], ss_c.at[k, h], rs_c.at[k, h], d_c)

    def start_if(condition, make, *args):
        @pl.when(condition)
        def _():
            make(*args).start()

    for h in range(2):
        wait_in(0, h)
        z_send(0, h).start()
        start_if(xh == 0, x_send, 0, 0, h)
        start_if(c == 0, c_send, 0, 0, h)
    w_x.wait_recv()
    for h in range(2):
        w_ring(0, 0, h).start()
    w_core(0, z).start()
    for j in range(2):
        wait_in(1, j)

    def got_z1(h):
        z_send(0, h).wait_recv()
        z_send(1, h).start()
        start_if(xh == 0, x_send, 2, 1, h)
        start_if(xh == 1, x_send, 2, 0, h)
        start_if(c == 0, c_send, 2, 1, h)
        start_if(c == 1, c_send, 2, 0, h)

    def got_a(h):
        x_send(0, 0, h).wait_recv()
        start_if(c == 0, c_send, 1, 2, h)
        start_if(c == 1, c_send, 1, 1, h)

    def got_z2(h):
        z_send(1, h).wait_recv()
        start_if(xh == 1, x_send, 4, 1, h)
        start_if(c == 1, c_send, 4, 2, h)

    def got_b(h):
        x_send(0, 1, h).wait_recv()
        c_send(3, 3, h).start()

    def got_c(k):
        for h in range(2):
            c_send(0, k, h).wait_recv()

    hg = 4 * z + 2 * xh + c
    scale = LOG2E / HS**0.5

    def bias(delta):
        return jnp.where(hg >= delta, 0.0, BIG).astype(F32)

    ones = jnp.ones((CH, HS), BF)

    def attend(j, segs, first=False):
        for g in range(4):
            for h in range(SH // ROWS):
                rows = slice(h * ROWS, (h + 1) * ROWS)
                q = qb[j, g, rows, :]
                scores, tops = [], []
                for ref, lo, size, mask, b in segs:
                    s = lax.dot_general(q, ref[0, lo : lo + size, :], NT, preferred_element_type=F32)
                    if mask is not None:
                        t = lax.broadcasted_iota(jnp.int32, s.shape, 0) + h * ROWS
                        k = lax.broadcasted_iota(jnp.int32, s.shape, 1)
                        s = jnp.where(k <= t if mask == "upto" else k > t, s, -BIG)
                    m = jnp.max(s, axis=1, keepdims=True)
                    scores.append(s)
                    tops.append(m if b is None else m - b)
                top = tops[0]
                for m in tops[1:]:
                    top = jnp.maximum(top, m)
                if first:
                    new = jnp.broadcast_to(top, (ROWS, HS))
                else:
                    old = mx[j, g, rows, :]
                    new = jnp.maximum(old, top)
                total = None
                for s, (ref, lo, size, mask, b) in zip(scores, segs):
                    m = new[:, :1] if b is None else new[:, :1] + b
                    p = jnp.exp2((s - m) * scale).astype(BF)
                    v = jnp.concatenate([ref[1, lo : lo + size, :], ones[:size]], 1)
                    u = jnp.dot(p, v, preferred_element_type=F32)
                    total = u if total is None else total + u
                if first:
                    acc[j, g, rows, :] = total
                else:
                    a = jnp.exp2((old - new) * scale)
                    acc[j, g, rows, :] = acc[j, g, rows, :] * jnp.concatenate([a, a], 1) + total
                mx[j, g, rows, :] = new

    def diagonal(j):
        last = (own.at[0], j * SH, SH, "upto", None)
        return [(own.at[0], 0, SH, None, None), last] if j else [last]

    def far(j):
        edge = (own.at[4], j * SH, SH, "after", bias(8))
        return [edge] if j else [edge, (own.at[4], SH, SH, None, bias(8))]

    def full(ref, delta):
        return (ref, 0, CH, None, bias(delta))

    odd = [jnp.where(c == 0, p, q) for p, q in ((3, 1), (1, 5), (7, 3), (5, 7))]

    yp, ym = lax.rem(y + 1, 4), lax.rem(y + 3, 4)

    def a_send(k, t):
        b = ab.at[y, t]
        return remote(b, b, ss_a.at[k, t], rs_a.at[k, t], dev(z, xh, ym if k else yp, xl, c))

    def a_relay(k, t):
        b = ab.at[yp if k else ym, t, pl.ds(k * 64, 64), :]
        return remote(b, b, ss_r.at[k, t], rs_r.at[k, t], dev(z, xh, ym if k else yp, xl, c))

    def a_start(t):
        for k in range(2):
            a_send(k, t).start()

    def a_got(t):
        for k in range(2):
            a_send(k, t).wait_recv()
            a_relay(k, t).start()

    def a_all(t):
        for k in range(2):
            a_relay(k, t).wait_recv()

    def finish(j):
        attend(j, [full(own.at[3], 6), full(oth.at[3], odd[3])])
        for h in range(2):
            rows = slice(h * ROWS, (h + 1) * ROWS)
            for g in range(4):
                a = acc[j, g, rows, :]
                ab[y, 2 * j + h, :, g * HS : (g + 1) * HS] = (a[:, :HS] / a[:, HS:]).astype(BF)

    def partial(t, side):
        total = None
        for yy in range(4):
            w = wb[yy // 2, pl.ds(side * 4, 4), :, :, (yy % 2) * CH : (yy % 2 + 1) * CH].reshape(CH, CH)
            u = lax.dot_general(ab[yy, t], w, NT, preferred_element_type=F32)
            total = u if total is None else total + u
        return total

    def p_send(t):
        return remote(pa.at[t], pr.at[t], ss_p.at[t], rs_p.at[t], d_l)

    def p_away(t):
        a_all(t)
        pa[t] = partial(t, 1 - xl).astype(BF)
        p_send(t).start()

    def p_own(t):
        pf[t] = partial(t, xl)

    def o_send(t, i):
        j, h = t // 2, t % 2
        place = out.at[y, pl.ds(h * ROWS, ROWS), :]
        return remote(rb.at[t, i], place, ss_o.at[t, i], rs_o.at[y, h], dev(z, xh, 2 * c + j, xl, i))

    def o_here(t, i):
        return jnp.logical_and(y == 2 * c + t // 2, c == i)

    def p_got(t):
        p_send(t).wait_recv()
        h = t % 2
        for i in range(2):
            cols = slice(i * SH, (i + 1) * SH)
            total = (pf[t, :, cols] + pr[t, :, cols].astype(F32)).astype(BF)

            @pl.when(o_here(t, i))
            def _():
                out[y, h * ROWS : (h + 1) * ROWS, :] = total

            @pl.when(jnp.logical_not(o_here(t, i)))
            def _():
                rb[t, i] = total
                o_send(t, i).start()

    got_z1(0)
    got_z1(1)
    for h in range(2):
        w_ring(1, 0, h).start()
    got_c(0)
    w_got(0, 0, 0)
    attend(0, diagonal(0) + [full(own.at[2], 4), full(oth.at[0], odd[0])], first=True)
    w_got(0, 0, 1)
    got_a(0)
    got_z2(0)
    attend(1, diagonal(1) + [full(own.at[2], 4), full(oth.at[0], odd[0])], first=True)
    got_a(1)
    got_z2(1)
    w_got(0, 1, 0)
    w_got(0, 1, 1)
    got_c(1)
    got_c(2)
    middle = [full(oth.at[1], odd[1]), full(oth.at[2], odd[2]), full(own.at[1], 2)]
    attend(0, middle + far(0))
    got_b(0)
    w_got(0, 2, 0)
    attend(1, middle + far(1))
    got_b(1)
    w_got(0, 2, 1)
    w_got(1, 0, 0)
    got_c(3)
    finish(0)
    a_start(0)
    a_start(1)
    w_got(1, 0, 1)
    w_got(0, 3, 0)
    finish(1)
    w_got(0, 3, 1)
    w_got(1, 1, 0)
    w_got(1, 1, 1)
    a_got(0)
    a_start(2)
    w_got(0, 4, 0)
    a_got(1)
    a_start(3)
    w_got(0, 4, 1)
    for k in range(8):
        w_core(k, z).wait_recv()
    p_away(0)
    a_got(2)
    p_own(0)
    p_away(1)
    p_own(1)
    a_got(3)
    p_got(0)
    p_away(2)
    p_own(2)
    p_got(1)
    p_away(3)
    p_own(3)
    p_got(2)
    p_got(3)

    for yy in range(4):
        @pl.when(jnp.logical_not(jnp.logical_and(yy == y, c == y // 2)))
        def _():
            for h in range(2):
                place = out.at[yy, pl.ds(h * ROWS, ROWS), :]
                remote(rb.at[0, 0], place, ss_o.at[0, 0], rs_o.at[yy, h], d_c).wait_recv()
    for i in range(2):
        @pl.when(is_remote(i))
        def _():
            for copy in to_head(i):
                copy.wait_send()
    w_x.wait_send()
    for h in range(2):
        for k in range(2):
            for n in range(UP if k else DOWN):
                w_ring(k, n, h).wait_send()
            z_send(k, h).wait_send()
            x_send(0, k, h).wait_send()
        for k in range(4):
            c_send(0, k, h).wait_send()
    for k in range(8):
        w_core(k, z).wait_send()
    for t in range(4):
        for k in range(2):
            a_send(k, t).wait_send()
            a_relay(k, t).wait_send()
        p_send(t).wait_send()
        for i in range(2):
            @pl.when(jnp.logical_not(o_here(t, i)))
            def _():
                o_send(t, i).wait_send()


def body(queries, keys, values, out_weight):
    tokens = queries.shape[0]
    q = queries.reshape(tokens, 2, 4, HS).transpose(1, 2, 0, 3)
    kv = jnp.stack([keys, values]).transpose(2, 0, 1, 3)
    dma = pltpu.SemaphoreType.DMA
    shapes = [(2,)] * 4 + [(2, 2)] * 4 + [(4, 2)] * 2 + [(1,)] * 2 + [(DOWN + UP, 2)] * 2 + [(8,)] * 2 + [(2, 4)] * 4 + [(4,)] * 2 + [(4, 2)] * 2
    sems = [dma(shape) for shape in shapes]
    vmem = pl.BlockSpec(memory_space=pltpu.VMEM)
    r = pl.pallas_call(
        kernel,
        name="layer",
        out_shape=jax.ShapeDtypeStruct((4, SH, SH), BF),
        in_specs=[vmem] * 3,
        out_specs=vmem,
        scratch_shapes=[
            pltpu.VMEM((2, 4, SH, HS), BF),
            pltpu.VMEM((5, 2, CH, HS), BF),
            pltpu.VMEM((4, 2, CH, HS), BF),
            pltpu.VMEM((2, 8, 2, 64, 1024), BF),
            pltpu.VMEM((2, 4, SH, HS), F32),
            pltpu.VMEM((2, 4, SH, 2 * HS), F32),
            pltpu.VMEM((4, 4, ROWS, CH), BF),
            pltpu.VMEM((4, ROWS, CH), F32),
            pltpu.VMEM((4, ROWS, CH), BF),
            pltpu.VMEM((4, ROWS, CH), BF),
            pltpu.VMEM((4, 2, ROWS, SH), BF),
            *sems,
        ],
        compiler_params=pltpu.CompilerParams(
            collective_id=0, has_side_effects=True, vmem_limit_bytes=48 * 2**20
        ),
    )(q, kv, out_weight.T)
    return r.reshape(4, tokens, 4, 64).transpose(1, 2, 0, 3).reshape(tokens, 1024)


def solution(mesh):
    return jax.shard_map(
        body,
        mesh=mesh,
        in_specs=(
            P("seq", "head", None),
            P("seq", "head", None),
            P("seq", "head", None),
            P("head", "seq"),
        ),
        out_specs=P("seq", "head"),
        check_vma=False,
    )
```

```python
import functools

import jax
import jax.numpy as jnp
from jax import lax
from jax.experimental import pallas as pl
from jax.experimental.pallas import tpu as pltpu
from jax.sharding import PartitionSpec as P

MESH = pl.DeviceIdType.MESH
NT = (((1,), (1,)), ((), ()))
BIG = 1e30
LOG2E = 1.4426950408889634
HS = 128
SH = 256
CH = 512
ROWS = 128
Q4 = 64
RING = [(0, s, h) for s in range(5) for h in range(2) if (s, h) != (4, 1)]
RING += [(1, s, h) for s in range(3) for h in range(2) if (s, h) != (2, 0)]
BF = jnp.bfloat16
F32 = jnp.float32


def kernel(
    q_in,
    kv_in,
    w_in,
    out,
    qb,
    own,
    oth,
    wb,
    mx,
    acc,
    ab,
    pf,
    pa,
    pr,
    rb,
    ss_kv, rs_kv, ss_q, rs_q,
    ss_z, rs_z, ss_x, rs_x,
    ss_c, rs_c,
    ss_wx, rs_wx,
    ss_w, rs_w,
    ss_wc, rs_wc,
    ss_a, rs_a,
    ss_r, rs_r,
    ss_p, rs_p,
    ss_o, rs_o,
):
    seq = lax.axis_index("seq")
    head = lax.axis_index("head")
    z, xh, y = seq // 8, (seq // 4) % 2, seq % 4
    xl, c = head // 2, head % 2

    def dev(zz, xx, yy, ll, cc):
        return (zz * 8 + xx * 4 + yy, ll * 2 + cc)

    zp, zm = lax.rem(z + 1, 8), lax.rem(z + 7, 8)
    d_zp = dev(zp, xh, y, xl, c)
    d_zm = dev(zm, xh, y, xl, c)
    d_x = dev(z, 1 - xh, y, xl, c)
    d_c = dev(z, xh, y, xl, 1 - c)
    d_l = dev(z, xh, y, 1 - xl, c)

    def remote(src, dst, ss, rs, device):
        return pltpu.make_async_remote_copy(
            src_ref=src, dst_ref=dst, send_sem=ss, recv_sem=rs,
            device_id=device, device_id_type=MESH,
        )

    barrier = pltpu.get_barrier_semaphore()
    for dy in range(4):
        for dc in range(2):
            if dy or dc:
                pl.semaphore_signal(
                    barrier, inc=1, device_id_type=MESH,
                    device_id=dev(z, xh, lax.rem(y + dy, 4), xl, lax.rem(c + dc, 2)),
                )
    for d in (d_zp, d_zm, d_x, d_l):
        pl.semaphore_signal(barrier, inc=1, device_id=d, device_id_type=MESH)
    pl.semaphore_wait(barrier, 11)

    jy = y % 2

    def to_head(i):
        dest = dev(z, xh, 2 * c + i, xl, y // 2)
        kv = remote(kv_in.at[i], own.at[0, :, pl.ds(jy * SH, SH), :], ss_kv.at[i], rs_kv.at[jy], dest)
        q = remote(q_in.at[i], qb.at[jy], ss_q.at[i], rs_q.at[jy], dest)
        return kv, q

    mine_here = c == y // 2

    def is_remote(i):
        return jnp.logical_not(jnp.logical_and(mine_here, jy == i))

    for i in range(2):
        @pl.when(is_remote(i))
        def _():
            to_head(i)[0].start()

    w_x = remote(w_in, wb.at[c, z, xh], ss_wx.at[0], rs_wx.at[0], d_x)
    w_x.start()
    wb[c, z, xh] = w_in[...]
    for i in range(2):
        @pl.when(is_remote(i))
        def _():
            to_head(i)[1].start()

    for i in range(2):
        @pl.when(jnp.logical_not(is_remote(i)))
        def _():
            own[0, :, i * SH : (i + 1) * SH, :] = kv_in[i]
            qb[i] = q_in[i]

    def wait_in(which, j):
        @pl.when(jnp.logical_not(jnp.logical_and(mine_here, jy == j)))
        def _():
            if which == 0:
                remote(kv_in.at[0], half(0, j), ss_kv.at[0], rs_kv.at[j], d_c).wait_recv()
            else:
                remote(q_in.at[0], qb.at[j], ss_q.at[0], rs_q.at[j], d_c).wait_recv()

    def w_ring(k, s, h):
        b = wb.at[c, lax.rem(z + s, 8) if k == 0 else lax.rem(z + 8 - s, 8), 1 - xh if h else xh]
        n = s if k == 0 else 5 + s
        return remote(b, b, ss_w.at[n, h], rs_w.at[n, h], d_zp if k else d_zm)

    def w_core(n, block):
        b = wb.at[c, block]
        return remote(b, b, ss_wc.at[n], rs_wc.at[n], d_c)

    def w_got(k, s, h):
        w_ring(k, s, h).wait_recv()
        if (k, s + 1, h) in RING:
            w_ring(k, s + 1, h).start()
        if h == 1 and s < (2 if k else 4):
            n = 5 + s if k else 1 + s
            w_core(n, lax.rem(z + 7 - s, 8) if k else lax.rem(z + 1 + s, 8)).start()

    def half(item, h):
        return own.at[item, :, pl.ds(h * SH, SH), :]

    def z_send(k, h):
        return remote(half(2 * k, h), half(2 * k + 2, h), ss_z.at[k, h], rs_z.at[k, h], d_zp)

    def x_send(item, k, h):
        return remote(half(item, h), half(1 + 2 * k, h), ss_x.at[k, h], rs_x.at[k, h], d_x)

    def c_send(item, k, h):
        return remote(half(item, h), oth.at[k, :, pl.ds(h * SH, SH), :], ss_c.at[k, h], rs_c.at[k, h], d_c)

    def start_if(condition, make, *args):
        @pl.when(condition)
        def _():
            make(*args).start()

    for k in range(2):
        w_ring(k, 0, 0).start()
    for h in range(2):
        wait_in(0, h)
        z_send(0, h).start()
        start_if(xh == 0, x_send, 0, 0, h)
        start_if(c == 0, c_send, 0, 0, h)
    w_x.wait_recv()
    w_ring(0, 0, 1).start()
    w_core(0, z).start()
    w_got(0, 0, 0)
    for j in range(2):
        wait_in(1, j)

    def got_z1(h):
        z_send(0, h).wait_recv()
        z_send(1, h).start()
        start_if(xh == 0, x_send, 2, 1, h)
        start_if(xh == 1, x_send, 2, 0, h)
        start_if(c == 0, c_send, 2, 1, h)
        start_if(c == 1, c_send, 2, 0, h)

    def got_a(h):
        x_send(0, 0, h).wait_recv()
        start_if(c == 0, c_send, 1, 2, h)
        start_if(c == 1, c_send, 1, 1, h)

    def got_z2(h):
        z_send(1, h).wait_recv()
        start_if(xh == 1, x_send, 4, 1, h)
        start_if(c == 1, c_send, 4, 2, h)

    def got_b(h):
        x_send(0, 1, h).wait_recv()
        c_send(3, 3, h).start()

    def got_c(k):
        for h in range(2):
            c_send(0, k, h).wait_recv()

    hg = 4 * z + 2 * xh + c
    scale = LOG2E / HS**0.5

    def bias(delta):
        return jnp.where(hg >= delta, 0.0, BIG).astype(F32)

    def attend(h, segs_of, first=False):
        rows = slice(h * ROWS, (h + 1) * ROWS)
        for j in range(2):
            segs = segs_of(j)
            keys = jnp.concatenate([ref[0, lo : lo + size, :] for ref, lo, size, _, _ in segs], 0)
            vals = jnp.concatenate([ref[1, lo : lo + size, :] for ref, lo, size, _, _ in segs], 0)
            vals = jnp.concatenate([vals, jnp.ones(vals.shape, BF)], 1)
            for g in range(4):
                every = lax.dot_general(qb[j, g, rows, :], keys, NT, preferred_element_type=F32)
                scores, tops, at = [], [], 0
                for _, _, size, mask, b in segs:
                    s = every[:, at : at + size]
                    at += size
                    if mask is not None:
                        t = lax.broadcasted_iota(jnp.int32, s.shape, 0) + h * ROWS
                        k = lax.broadcasted_iota(jnp.int32, s.shape, 1)
                        s = jnp.where(k <= t if mask == "upto" else k > t, s, -BIG)
                    m = jnp.max(s, axis=1, keepdims=True)
                    scores.append(s)
                    tops.append(m if b is None else m - b)
                top = functools.reduce(jnp.maximum, tops)
                if first:
                    new = jnp.broadcast_to(top, (ROWS, HS))
                else:
                    old = mx[j, g, rows, :]
                    new = jnp.maximum(old, top)
                probs = []
                for s, (_, _, _, _, b) in zip(scores, segs):
                    m = new[:, :1] if b is None else new[:, :1] + b
                    probs.append(jnp.exp2((s - m) * scale).astype(BF))
                total = jnp.dot(jnp.concatenate(probs, 1), vals, preferred_element_type=F32)
                if first:
                    acc[j, g, rows, :] = total
                else:
                    a = jnp.exp2((old - new) * scale)
                    acc[j, g, rows, :] = acc[j, g, rows, :] * jnp.concatenate([a, a], 1) + total
                mx[j, g, rows, :] = new

    def diagonal(j):
        last = (own.at[0], j * SH, SH, "upto", None)
        return [(own.at[0], 0, SH, None, None), last] if j else [last]

    def far(j):
        edge = (own.at[4], j * SH, SH, "after", bias(8))
        return [edge] if j else [edge, (own.at[4], SH, SH, None, bias(8))]

    def full(ref, delta):
        return (ref, 0, CH, None, bias(delta))

    odd = [jnp.where(c == 0, p, q) for p, q in ((3, 1), (1, 5), (7, 3), (5, 7))]

    yp, ym = lax.rem(y + 1, 4), lax.rem(y + 3, 4)

    def a_send(k, t):
        b = ab.at[y, t]
        return remote(b, b, ss_a.at[k, t], rs_a.at[k, t], dev(z, xh, ym if k else yp, xl, c))

    def a_relay(k, t):
        b = ab.at[yp if k else ym, t, pl.ds(k * 64, 64), :]
        return remote(b, b, ss_r.at[k, t], rs_r.at[k, t], dev(z, xh, ym if k else yp, xl, c))

    def a_start(t):
        for k in range(2):
            a_send(k, t).start()

    def a_got(t):
        for k in range(2):
            a_send(k, t).wait_recv()
            a_relay(k, t).start()

    def a_all(t):
        for k in range(2):
            a_relay(k, t).wait_recv()

    def finish(h):
        attend(h, lambda j: [full(own.at[3], 6), full(oth.at[3], odd[3])])
        rows = slice(h * ROWS, (h + 1) * ROWS)
        for j in range(2):
            for g in range(4):
                a = acc[j, g, rows, :]
                a = (a[:, :HS] / a[:, HS:]).astype(BF)
                for t in range(2):
                    ab[y, 2 * h + t, j * Q4 : (j + 1) * Q4, g * HS : (g + 1) * HS] = a[t * Q4 : (t + 1) * Q4]

    def partial(t, side):
        total = None
        for yy in range(4):
            w = wb[yy // 2, pl.ds(side * 4, 4), :, :, (yy % 2) * CH : (yy % 2 + 1) * CH].reshape(CH, CH)
            u = lax.dot_general(ab[yy, t], w, NT, preferred_element_type=F32)
            total = u if total is None else total + u
        return total

    def p_send(t):
        return remote(pa.at[t], pr.at[t], ss_p.at[t], rs_p.at[t], d_l)

    def p_away(t):
        a_all(t)
        pa[t] = partial(t, 1 - xl).astype(BF)
        p_send(t).start()

    def p_own(t):
        pf[t] = partial(t, xl)

    def o_send(t, j, i):
        place = out.at[y, pl.ds(t * Q4, Q4), :]
        return remote(rb.at[t, i, pl.ds(j * Q4, Q4), :], place, ss_o.at[t, 2 * j + i], rs_o.at[y, t], dev(z, xh, 2 * c + j, xl, i))

    def o_here(j, i):
        return jnp.logical_and(y == 2 * c + j, c == i)

    def p_got(t):
        p_send(t).wait_recv()
        for i in range(2):
            cols = slice(i * SH, (i + 1) * SH)
            rb[t, i] = (pf[t, :, cols] + pr[t, :, cols].astype(F32)).astype(BF)
        for j in range(2):
            for i in range(2):
                @pl.when(o_here(j, i))
                def _():
                    out[y, t * Q4 : (t + 1) * Q4, :] = rb[t, i, j * Q4 : (j + 1) * Q4, :]

                @pl.when(jnp.logical_not(o_here(j, i)))
                def _():
                    o_send(t, j, i).start()

    def near(j):
        return diagonal(j) + [full(own.at[2], 4), full(oth.at[0], odd[0])]

    def middle(j):
        return [full(own.at[1], 2), full(oth.at[1], odd[1]), full(oth.at[2], odd[2])] + far(j)

    got_z1(0)
    got_z1(1)
    w_ring(1, 0, 1).start()
    w_got(1, 0, 0)
    w_got(0, 0, 1)
    got_c(0)
    attend(0, near, first=True)
    w_got(0, 1, 0)
    got_a(0)
    got_z2(0)
    w_got(0, 1, 1)
    attend(1, near, first=True)
    got_a(1)
    got_z2(1)
    w_got(0, 2, 0)
    got_c(1)
    got_c(2)
    attend(0, middle)
    got_b(0)
    got_b(1)
    w_got(0, 2, 1)
    w_got(1, 0, 1)
    w_got(1, 1, 0)
    w_got(0, 3, 0)
    got_c(3)
    finish(0)
    a_start(0)
    a_start(1)
    w_got(1, 1, 1)
    attend(1, middle)
    w_got(0, 3, 1)
    w_got(0, 4, 0)
    a_got(0)
    finish(1)
    a_start(2)
    a_got(1)
    a_start(3)
    w_got(1, 2, 1)
    w_core(7, lax.rem(z + 5, 8)).start()
    for k in range(8):
        w_core(k, z).wait_recv()
    p_away(0)
    p_own(0)
    a_got(2)
    p_away(1)
    p_own(1)
    a_got(3)
    p_got(0)
    p_away(2)
    p_own(2)
    p_got(1)
    p_away(3)
    p_own(3)
    p_got(2)
    p_got(3)

    for yy in range(4):
        @pl.when(jnp.logical_not(jnp.logical_and(yy == y, c == y // 2)))
        def _():
            for t in range(4):
                place = out.at[yy, pl.ds(t * Q4, Q4), :]
                remote(rb.at[0, 0, pl.ds(0, Q4), :], place, ss_o.at[0, 0], rs_o.at[yy, t], d_c).wait_recv()
    for i in range(2):
        @pl.when(is_remote(i))
        def _():
            for copy in to_head(i):
                copy.wait_send()
    w_x.wait_send()
    for k, n, h in RING:
        w_ring(k, n, h).wait_send()
    for h in range(2):
        for k in range(2):
            z_send(k, h).wait_send()
            x_send(0, k, h).wait_send()
        for k in range(4):
            c_send(0, k, h).wait_send()
    for k in range(8):
        w_core(k, z).wait_send()
    for t in range(4):
        for k in range(2):
            a_send(k, t).wait_send()
            a_relay(k, t).wait_send()
        p_send(t).wait_send()
        for j in range(2):
            for i in range(2):
                @pl.when(jnp.logical_not(o_here(j, i)))
                def _():
                    o_send(t, j, i).wait_send()


def body(queries, keys, values, out_weight):
    tokens = queries.shape[0]
    q = queries.reshape(tokens, 2, 4, HS).transpose(1, 2, 0, 3)
    kv = jnp.stack([keys, values]).transpose(2, 0, 1, 3)
    dma = pltpu.SemaphoreType.DMA
    shapes = [(2,)] * 4 + [(2, 2)] * 4 + [(4, 2)] * 2 + [(1,)] * 2 + [(8, 2)] * 2 + [(8,)] * 2 + [(2, 4)] * 4 + [(4,)] * 2 + [(4, 4)] * 2
    sems = [dma(shape) for shape in shapes]
    vmem = pl.BlockSpec(memory_space=pltpu.VMEM)
    r = pl.pallas_call(
        kernel,
        name="layer",
        out_shape=jax.ShapeDtypeStruct((4, SH, SH), BF),
        in_specs=[vmem] * 3,
        out_specs=vmem,
        scratch_shapes=[
            pltpu.VMEM((2, 4, SH, HS), BF),
            pltpu.VMEM((5, 2, CH, HS), BF),
            pltpu.VMEM((4, 2, CH, HS), BF),
            pltpu.VMEM((2, 8, 2, 64, 1024), BF),
            pltpu.VMEM((2, 4, SH, HS), F32),
            pltpu.VMEM((2, 4, SH, 2 * HS), F32),
            pltpu.VMEM((4, 4, ROWS, CH), BF),
            pltpu.VMEM((4, ROWS, CH), F32),
            pltpu.VMEM((4, ROWS, CH), BF),
            pltpu.VMEM((4, ROWS, CH), BF),
            pltpu.VMEM((4, 2, ROWS, SH), BF),
            *sems,
        ],
        compiler_params=pltpu.CompilerParams(
            collective_id=0, has_side_effects=True, vmem_limit_bytes=48 * 2**20
        ),
    )(q, kv, out_weight.T)
    return r.reshape(4, tokens, 4, 64).transpose(1, 2, 0, 3).reshape(tokens, 1024)


def solution(mesh):
    return jax.shard_map(
        body,
        mesh=mesh,
        in_specs=(
            P("seq", "head", None),
            P("seq", "head", None),
            P("seq", "head", None),
            P("head", "seq"),
        ),
        out_specs=P("seq", "head"),
        check_vma=False,
    )
```

```python
import functools

import jax
import jax.numpy as jnp
from jax import lax
from jax.experimental import pallas as pl
from jax.experimental.pallas import tpu as pltpu
from jax.sharding import PartitionSpec as P

MESH = pl.DeviceIdType.MESH
NT = (((1,), (1,)), ((), ()))
BIG = 1e30
LOG2E = 1.4426950408889634
HS = 128
SH = 256
CH = 512
ROWS = 128
PIECES = [(0, 0, 64), (0, 64, 64), (1, 128, 64), (1, 192, 32), (1, 224, 32)]
RING = [(0, s, h) for s in range(5) for h in range(2) if (s, h) != (4, 1)]
RING += [(1, s, h) for s in range(3) for h in range(2) if (s, h) != (2, 0)]
BF = jnp.bfloat16
F32 = jnp.float32


def kernel(
    q_in,
    kv_in,
    w_in,
    out,
    qb,
    own,
    oth,
    wb,
    mx,
    acc,
    ab,
    pf,
    pa,
    pr,
    rb,
    ss_kv, rs_kv, ss_q, rs_q,
    ss_z, rs_z, ss_x, rs_x,
    ss_c, rs_c,
    ss_wx, rs_wx,
    ss_w, rs_w,
    ss_wc, rs_wc,
    ss_a, rs_a,
    ss_r, rs_r,
    ss_p, rs_p,
    ss_o, rs_o,
):
    seq = lax.axis_index("seq")
    head = lax.axis_index("head")
    z, xh, y = seq // 8, (seq // 4) % 2, seq % 4
    xl, c = head // 2, head % 2

    def dev(zz, xx, yy, ll, cc):
        return (zz * 8 + xx * 4 + yy, ll * 2 + cc)

    zp, zm = lax.rem(z + 1, 8), lax.rem(z + 7, 8)
    d_zp = dev(zp, xh, y, xl, c)
    d_zm = dev(zm, xh, y, xl, c)
    d_x = dev(z, 1 - xh, y, xl, c)
    d_c = dev(z, xh, y, xl, 1 - c)
    d_l = dev(z, xh, y, 1 - xl, c)

    def remote(src, dst, ss, rs, device):
        return pltpu.make_async_remote_copy(
            src_ref=src, dst_ref=dst, send_sem=ss, recv_sem=rs,
            device_id=device, device_id_type=MESH,
        )

    barrier = pltpu.get_barrier_semaphore()
    for dy in range(4):
        for dc in range(2):
            if dy or dc:
                pl.semaphore_signal(
                    barrier, inc=1, device_id_type=MESH,
                    device_id=dev(z, xh, lax.rem(y + dy, 4), xl, lax.rem(c + dc, 2)),
                )
    for d in (d_zp, d_zm, d_x, d_l):
        pl.semaphore_signal(barrier, inc=1, device_id=d, device_id_type=MESH)
    pl.semaphore_wait(barrier, 11)

    jy = y % 2

    def to_head(i):
        dest = dev(z, xh, 2 * c + i, xl, y // 2)
        kv = remote(kv_in.at[i], own.at[0, :, pl.ds(jy * SH, SH), :], ss_kv.at[i], rs_kv.at[jy], dest)
        q = remote(q_in.at[i], qb.at[jy], ss_q.at[i], rs_q.at[jy], dest)
        return kv, q

    mine_here = c == y // 2

    def is_remote(i):
        return jnp.logical_not(jnp.logical_and(mine_here, jy == i))

    for i in range(2):
        @pl.when(is_remote(i))
        def _():
            to_head(i)[0].start()

    w_x = remote(w_in, wb.at[c, z, xh], ss_wx.at[0], rs_wx.at[0], d_x)
    w_x.start()
    wb[c, z, xh] = w_in[...]
    for i in range(2):
        @pl.when(is_remote(i))
        def _():
            to_head(i)[1].start()

    for i in range(2):
        @pl.when(jnp.logical_not(is_remote(i)))
        def _():
            own[0, :, i * SH : (i + 1) * SH, :] = kv_in[i]
            qb[i] = q_in[i]

    def wait_in(which, j):
        @pl.when(jnp.logical_not(jnp.logical_and(mine_here, jy == j)))
        def _():
            if which == 0:
                remote(kv_in.at[0], half(0, j), ss_kv.at[0], rs_kv.at[j], d_c).wait_recv()
            else:
                remote(q_in.at[0], qb.at[j], ss_q.at[0], rs_q.at[j], d_c).wait_recv()

    def w_ring(k, s, h):
        b = wb.at[c, lax.rem(z + s, 8) if k == 0 else lax.rem(z + 8 - s, 8), 1 - xh if h else xh]
        n = s if k == 0 else 5 + s
        return remote(b, b, ss_w.at[n, h], rs_w.at[n, h], d_zp if k else d_zm)

    def w_core(n, block):
        b = wb.at[c, block]
        return remote(b, b, ss_wc.at[n], rs_wc.at[n], d_c)

    def w_got(k, s, h):
        w_ring(k, s, h).wait_recv()
        if (k, s + 1, h) in RING:
            w_ring(k, s + 1, h).start()
        if h == 1 and s < (2 if k else 4):
            n = 5 + s if k else 1 + s
            w_core(n, lax.rem(z + 7 - s, 8) if k else lax.rem(z + 1 + s, 8)).start()

    def half(item, h):
        return own.at[item, :, pl.ds(h * SH, SH), :]

    def z_send(k, h):
        return remote(half(2 * k, h), half(2 * k + 2, h), ss_z.at[k, h], rs_z.at[k, h], d_zp)

    def x_send(item, k, h):
        return remote(half(item, h), half(1 + 2 * k, h), ss_x.at[k, h], rs_x.at[k, h], d_x)

    def c_send(item, k, h):
        return remote(half(item, h), oth.at[k, :, pl.ds(h * SH, SH), :], ss_c.at[k, h], rs_c.at[k, h], d_c)

    def start_if(condition, make, *args):
        @pl.when(condition)
        def _():
            make(*args).start()

    for k in range(2):
        w_ring(k, 0, 0).start()
    for h in range(2):
        wait_in(0, h)
        z_send(0, h).start()
        start_if(xh == 0, x_send, 0, 0, h)
        start_if(c == 0, c_send, 0, 0, h)
    w_x.wait_recv()
    w_ring(0, 0, 1).start()
    w_core(0, z).start()
    w_got(0, 0, 0)
    for j in range(2):
        wait_in(1, j)

    def got_z1(h):
        z_send(0, h).wait_recv()
        z_send(1, h).start()
        start_if(xh == 0, x_send, 2, 1, h)
        start_if(xh == 1, x_send, 2, 0, h)
        start_if(c == 0, c_send, 2, 1, h)
        start_if(c == 1, c_send, 2, 0, h)

    def got_a(h):
        x_send(0, 0, h).wait_recv()
        start_if(c == 0, c_send, 1, 2, h)
        start_if(c == 1, c_send, 1, 1, h)

    def got_z2(h):
        z_send(1, h).wait_recv()
        start_if(xh == 1, x_send, 4, 1, h)
        start_if(c == 1, c_send, 4, 2, h)

    def got_b(h):
        x_send(0, 1, h).wait_recv()
        c_send(3, 3, h).start()

    def got_c(k):
        for h in range(2):
            c_send(0, k, h).wait_recv()

    hg = 4 * z + 2 * xh + c
    scale = LOG2E / HS**0.5

    def bias(delta):
        return jnp.where(hg >= delta, 0.0, BIG).astype(F32)

    def attend(h, segs_of, first=False):
        rows = slice(h * ROWS, (h + 1) * ROWS)
        for j in range(2):
            segs = segs_of(j)
            keys = jnp.concatenate([ref[0, lo : lo + size, :] for ref, lo, size, _, _ in segs], 0)
            vals = jnp.concatenate([ref[1, lo : lo + size, :] for ref, lo, size, _, _ in segs], 0)
            vals = jnp.concatenate([vals, jnp.ones(vals.shape, BF)], 1)
            for g in range(4):
                every = lax.dot_general(qb[j, g, rows, :], keys, NT, preferred_element_type=F32)
                scores, tops, at = [], [], 0
                for _, _, size, mask, b in segs:
                    s = every[:, at : at + size]
                    at += size
                    if mask is not None:
                        t = lax.broadcasted_iota(jnp.int32, s.shape, 0) + h * ROWS
                        k = lax.broadcasted_iota(jnp.int32, s.shape, 1)
                        s = jnp.where(k <= t if mask == "upto" else k > t, s, -BIG)
                    m = jnp.max(s, axis=1, keepdims=True)
                    scores.append(s)
                    tops.append(m if b is None else m - b)
                top = functools.reduce(jnp.maximum, tops)
                if first:
                    new = jnp.broadcast_to(top, (ROWS, HS))
                else:
                    old = mx[j, g, rows, :]
                    new = jnp.maximum(old, top)
                probs = []
                for s, (_, _, _, _, b) in zip(scores, segs):
                    m = new[:, :1] if b is None else new[:, :1] + b
                    probs.append(jnp.exp2((s - m) * scale).astype(BF))
                total = jnp.dot(jnp.concatenate(probs, 1), vals, preferred_element_type=F32)
                if first:
                    acc[j, g, rows, :] = total
                else:
                    a = jnp.exp2((old - new) * scale)
                    acc[j, g, rows, :] = acc[j, g, rows, :] * jnp.concatenate([a, a], 1) + total
                mx[j, g, rows, :] = new

    def diagonal(j):
        last = (own.at[0], j * SH, SH, "upto", None)
        return [(own.at[0], 0, SH, None, None), last] if j else [last]

    def far(j):
        edge = (own.at[4], j * SH, SH, "after", bias(8))
        return [edge] if j else [edge, (own.at[4], SH, SH, None, bias(8))]

    def full(ref, delta):
        return (ref, 0, CH, None, bias(delta))

    odd = [jnp.where(c == 0, p, q) for p, q in ((3, 1), (1, 5), (7, 3), (5, 7))]

    yp, ym = lax.rem(y + 1, 4), lax.rem(y + 3, 4)

    def piece(t):
        _, lo, n = PIECES[t]
        return slice(2 * lo, 2 * (lo + n)), pl.ds(2 * lo, 2 * n)

    def a_send(k, t):
        b = ab.at[y, piece(t)[1], :]
        return remote(b, b, ss_a.at[k, t], rs_a.at[k, t], dev(z, xh, ym if k else yp, xl, c))

    def a_relay(k, t):
        _, lo, n = PIECES[t]
        b = ab.at[yp if k else ym, pl.ds(2 * lo + k * n, n), :]
        return remote(b, b, ss_r.at[k, t], rs_r.at[k, t], dev(z, xh, ym if k else yp, xl, c))

    def a_start(t):
        for k in range(2):
            a_send(k, t).start()

    def a_got(t):
        for k in range(2):
            a_send(k, t).wait_recv()
            a_relay(k, t).start()

    def a_all(t):
        for k in range(2):
            a_relay(k, t).wait_recv()

    def finish(h):
        attend(h, lambda j: [full(own.at[3], 6), full(oth.at[3], odd[3])])
        rows = slice(h * ROWS, (h + 1) * ROWS)
        for j in range(2):
            for g in range(4):
                a = acc[j, g, rows, :]
                a = (a[:, :HS] / a[:, HS:]).astype(BF)
                for p, lo, n in PIECES:
                    if p == h:
                        row, tok = 2 * lo + j * n, lo - h * ROWS
                        ab[y, row : row + n, g * HS : (g + 1) * HS] = a[tok : tok + n]

    def partial(t, side):
        total = None
        for yy in range(4):
            w = wb[yy // 2, pl.ds(side * 4, 4), :, :, (yy % 2) * CH : (yy % 2 + 1) * CH].reshape(CH, CH)
            u = lax.dot_general(ab[yy, piece(t)[0], :], w, NT, preferred_element_type=F32)
            total = u if total is None else total + u
        return total

    def p_send(t):
        rows = piece(t)[1]
        return remote(pa.at[rows, :], pr.at[rows, :], ss_p.at[t], rs_p.at[t], d_l)

    def p_away(t):
        a_all(t)
        pa[piece(t)[0], :] = partial(t, 1 - xl).astype(BF)
        p_send(t).start()

    def p_own(t):
        pf[piece(t)[0], :] = partial(t, xl)

    def o_send(t, j, i):
        _, lo, n = PIECES[t]
        source, place = rb.at[i, pl.ds(2 * lo + j * n, n), :], out.at[y, pl.ds(lo, n), :]
        return remote(source, place, ss_o.at[t, 2 * j + i], rs_o.at[y, t], dev(z, xh, 2 * c + j, xl, i))

    def o_here(j, i):
        return jnp.logical_and(y == 2 * c + j, c == i)

    def p_got(t):
        p_send(t).wait_recv()
        rows = piece(t)[0]
        _, lo, n = PIECES[t]
        for i in range(2):
            cols = slice(i * SH, (i + 1) * SH)
            rb[i, rows, :] = (pf[rows, cols] + pr[rows, cols].astype(F32)).astype(BF)
        for j in range(2):
            for i in range(2):
                @pl.when(o_here(j, i))
                def _():
                    out[y, lo : lo + n, :] = rb[i, 2 * lo + j * n : 2 * lo + (j + 1) * n, :]

                @pl.when(jnp.logical_not(o_here(j, i)))
                def _():
                    o_send(t, j, i).start()

    def near(j):
        return diagonal(j) + [full(own.at[2], 4), full(oth.at[0], odd[0])]

    def middle(j):
        return [full(own.at[1], 2), full(oth.at[1], odd[1]), full(oth.at[2], odd[2])] + far(j)

    got_z1(0)
    got_z1(1)
    w_ring(1, 0, 1).start()
    w_got(1, 0, 0)
    w_got(0, 0, 1)
    got_c(0)
    attend(0, near, first=True)
    w_got(0, 1, 0)
    got_a(0)
    got_z2(0)
    w_got(0, 1, 1)
    attend(1, near, first=True)
    got_a(1)
    got_z2(1)
    w_got(0, 2, 0)
    got_c(1)
    got_c(2)
    attend(0, middle)
    got_b(0)
    got_b(1)
    w_got(0, 2, 1)
    w_got(1, 0, 1)
    w_got(1, 1, 0)
    w_got(0, 3, 0)
    got_c(3)
    finish(0)
    a_start(0)
    a_start(1)
    attend(1, middle)
    w_got(1, 1, 1)
    w_got(0, 3, 1)
    finish(1)
    a_got(0)
    a_start(2)
    w_got(0, 4, 0)
    a_got(1)
    a_start(3)
    w_got(1, 2, 1)
    w_core(7, lax.rem(z + 5, 8)).start()
    for k in range(8):
        w_core(k, z).wait_recv()
    p_away(0)
    p_own(0)
    a_got(2)
    a_start(4)
    p_away(1)
    a_got(3)
    p_own(1)
    p_got(0)
    p_away(2)
    a_got(4)
    p_own(2)
    p_away(3)
    p_own(3)
    p_got(1)
    p_away(4)
    p_own(4)
    for t in range(2, 5):
        p_got(t)

    for yy in range(4):
        @pl.when(jnp.logical_not(jnp.logical_and(yy == y, c == y // 2)))
        def _():
            for t, (_, lo, n) in enumerate(PIECES):
                place = out.at[yy, pl.ds(lo, n), :]
                remote(rb.at[0, pl.ds(lo, n), :], place, ss_o.at[0, 0], rs_o.at[yy, t], d_c).wait_recv()
    for i in range(2):
        @pl.when(is_remote(i))
        def _():
            for copy in to_head(i):
                copy.wait_send()
    w_x.wait_send()
    for k, n, h in RING:
        w_ring(k, n, h).wait_send()
    for h in range(2):
        for k in range(2):
            z_send(k, h).wait_send()
            x_send(0, k, h).wait_send()
        for k in range(4):
            c_send(0, k, h).wait_send()
    for k in range(8):
        w_core(k, z).wait_send()
    for t in range(len(PIECES)):
        for k in range(2):
            a_send(k, t).wait_send()
            a_relay(k, t).wait_send()
        p_send(t).wait_send()
        for j in range(2):
            for i in range(2):
                @pl.when(jnp.logical_not(o_here(j, i)))
                def _():
                    o_send(t, j, i).wait_send()


def body(queries, keys, values, out_weight):
    tokens = queries.shape[0]
    q = queries.reshape(tokens, 2, 4, HS).transpose(1, 2, 0, 3)
    kv = jnp.stack([keys, values]).transpose(2, 0, 1, 3)
    dma = pltpu.SemaphoreType.DMA
    shapes = [(2,)] * 4 + [(2, 2)] * 4 + [(4, 2)] * 2 + [(1,)] * 2 + [(8, 2)] * 2 + [(8,)] * 2 + [(2, 5)] * 4 + [(5,)] * 2 + [(5, 4), (4, 5)]
    sems = [dma(shape) for shape in shapes]
    vmem = pl.BlockSpec(memory_space=pltpu.VMEM)
    r = pl.pallas_call(
        kernel,
        name="layer",
        out_shape=jax.ShapeDtypeStruct((4, SH, SH), BF),
        in_specs=[vmem] * 3,
        out_specs=vmem,
        scratch_shapes=[
            pltpu.VMEM((2, 4, SH, HS), BF),
            pltpu.VMEM((5, 2, CH, HS), BF),
            pltpu.VMEM((4, 2, CH, HS), BF),
            pltpu.VMEM((2, 8, 2, 64, 1024), BF),
            pltpu.VMEM((2, 4, SH, HS), F32),
            pltpu.VMEM((2, 4, SH, 2 * HS), F32),
            pltpu.VMEM((4, CH, CH), BF),
            pltpu.VMEM((CH, CH), F32),
            pltpu.VMEM((CH, CH), BF),
            pltpu.VMEM((CH, CH), BF),
            pltpu.VMEM((2, CH, SH), BF),
            *sems,
        ],
        compiler_params=pltpu.CompilerParams(
            collective_id=0, has_side_effects=True, vmem_limit_bytes=48 * 2**20
        ),
    )(q, kv, out_weight.T)
    return r.reshape(4, tokens, 4, 64).transpose(1, 2, 0, 3).reshape(tokens, 1024)


def solution(mesh):
    return jax.shard_map(
        body,
        mesh=mesh,
        in_specs=(
            P("seq", "head", None),
            P("seq", "head", None),
            P("seq", "head", None),
            P("head", "seq"),
        ),
        out_specs=P("seq", "head"),
        check_vma=False,
    )
```

```python
import functools

import jax
import jax.numpy as jnp
from jax import lax
from jax.experimental import pallas as pl
from jax.experimental.pallas import tpu as pltpu
from jax.sharding import PartitionSpec as P

MESH = pl.DeviceIdType.MESH
NT = (((1,), (1,)), ((), ()))
BIG = 1e30
LOG2E = 1.4426950408889634
HS = 128
SH = 256
CH = 512
ROWS = 128
PIECES = [(0, 0, 64), (0, 64, 64), (1, 128, 64), (1, 192, 32), (1, 224, 32)]
RING = [(0, s, h) for s in range(5) for h in range(2) if (s, h) != (4, 1)]
RING += [(1, s, h) for s in range(3) for h in range(2) if (s, h) != (2, 0)]
BF = jnp.bfloat16
F32 = jnp.float32


def kernel(
    q_in,
    kv_in,
    w_in,
    out,
    qb,
    own,
    oth,
    wb,
    mx,
    acc,
    ab,
    pf,
    pa,
    pr,
    rb,
    ss_kv, rs_kv, ss_q, rs_q,
    ss_z, rs_z, ss_x, rs_x,
    ss_c, rs_c,
    ss_wx, rs_wx,
    ss_w, rs_w,
    ss_wc, rs_wc,
    ss_a, rs_a,
    ss_r, rs_r,
    ss_p, rs_p,
    ss_o, rs_o,
):
    seq = lax.axis_index("seq")
    head = lax.axis_index("head")
    z, xh, y = seq // 8, (seq // 4) % 2, seq % 4
    xl, c = head // 2, head % 2

    def dev(zz, xx, yy, ll, cc):
        return (zz * 8 + xx * 4 + yy, ll * 2 + cc)

    zp, zm = lax.rem(z + 1, 8), lax.rem(z + 7, 8)
    d_zp = dev(zp, xh, y, xl, c)
    d_zm = dev(zm, xh, y, xl, c)
    d_x = dev(z, 1 - xh, y, xl, c)
    d_c = dev(z, xh, y, xl, 1 - c)
    d_l = dev(z, xh, y, 1 - xl, c)

    def remote(src, dst, ss, rs, device):
        return pltpu.make_async_remote_copy(
            src_ref=src, dst_ref=dst, send_sem=ss, recv_sem=rs,
            device_id=device, device_id_type=MESH,
        )

    barrier = pltpu.get_barrier_semaphore()
    for dy in range(4):
        for dc in range(2):
            if dy or dc:
                pl.semaphore_signal(
                    barrier, inc=1, device_id_type=MESH,
                    device_id=dev(z, xh, lax.rem(y + dy, 4), xl, lax.rem(c + dc, 2)),
                )
    for d in (d_zp, d_zm, d_x, d_l):
        pl.semaphore_signal(barrier, inc=1, device_id=d, device_id_type=MESH)
    pl.semaphore_wait(barrier, 11)

    jy = y % 2

    def to_head(i):
        dest = dev(z, xh, 2 * c + i, xl, y // 2)
        kv = remote(kv_in.at[i], own.at[0, :, pl.ds(jy * SH, SH), :], ss_kv.at[i], rs_kv.at[jy], dest)
        q = remote(q_in.at[i], qb.at[jy], ss_q.at[i], rs_q.at[jy], dest)
        return kv, q

    mine_here = c == y // 2

    def is_remote(i):
        return jnp.logical_not(jnp.logical_and(mine_here, jy == i))

    for i in range(2):
        @pl.when(is_remote(i))
        def _():
            to_head(i)[0].start()

    w_x = remote(w_in, wb.at[c, z, xh], ss_wx.at[0], rs_wx.at[0], d_x)
    w_x.start()
    wb[c, z, xh] = w_in[...]
    for i in range(2):
        @pl.when(is_remote(i))
        def _():
            to_head(i)[1].start()

    for i in range(2):
        @pl.when(jnp.logical_not(is_remote(i)))
        def _():
            own[0, :, i * SH : (i + 1) * SH, :] = kv_in[i]
            qb[i] = q_in[i]

    def wait_in(which, j):
        @pl.when(jnp.logical_not(jnp.logical_and(mine_here, jy == j)))
        def _():
            if which == 0:
                remote(kv_in.at[0], half(0, j), ss_kv.at[0], rs_kv.at[j], d_c).wait_recv()
            else:
                remote(q_in.at[0], qb.at[j], ss_q.at[0], rs_q.at[j], d_c).wait_recv()

    def w_ring(k, s, h):
        b = wb.at[c, lax.rem(z + s, 8) if k == 0 else lax.rem(z + 8 - s, 8), 1 - xh if h else xh]
        n = s if k == 0 else 5 + s
        return remote(b, b, ss_w.at[n, h], rs_w.at[n, h], d_zp if k else d_zm)

    def w_core(n, block):
        b = wb.at[c, block]
        return remote(b, b, ss_wc.at[n], rs_wc.at[n], d_c)

    def w_got(k, s, h):
        w_ring(k, s, h).wait_recv()
        if (k, s + 1, h) in RING:
            w_ring(k, s + 1, h).start()
        if h == 1 and s < (2 if k else 4):
            n = 5 + s if k else 1 + s
            w_core(n, lax.rem(z + 7 - s, 8) if k else lax.rem(z + 1 + s, 8)).start()

    def half(item, h):
        return own.at[item, :, pl.ds(h * SH, SH), :]

    def z_send(k, h):
        return remote(half(2 * k, h), half(2 * k + 2, h), ss_z.at[k, h], rs_z.at[k, h], d_zp)

    def x_send(item, k, h):
        return remote(half(item, h), half(1 + 2 * k, h), ss_x.at[k, h], rs_x.at[k, h], d_x)

    def c_send(item, k, h):
        return remote(half(item, h), oth.at[k, :, pl.ds(h * SH, SH), :], ss_c.at[k, h], rs_c.at[k, h], d_c)

    def start_if(condition, make, *args):
        @pl.when(condition)
        def _():
            make(*args).start()

    for k in range(2):
        w_ring(k, 0, 0).start()
    for h in range(2):
        wait_in(0, h)
        z_send(0, h).start()
        start_if(xh == 0, x_send, 0, 0, h)
        start_if(c == 0, c_send, 0, 0, h)
    w_x.wait_recv()
    w_ring(0, 0, 1).start()
    w_core(0, z).start()
    w_got(0, 0, 0)
    for j in range(2):
        wait_in(1, j)

    def got_z1(h):
        z_send(0, h).wait_recv()
        z_send(1, h).start()
        start_if(xh == 0, x_send, 2, 1, h)
        start_if(xh == 1, x_send, 2, 0, h)
        start_if(c == 0, c_send, 2, 1, h)
        start_if(c == 1, c_send, 2, 0, h)

    def got_a(h):
        x_send(0, 0, h).wait_recv()
        start_if(c == 0, c_send, 1, 2, h)
        start_if(c == 1, c_send, 1, 1, h)

    def got_z2(h):
        z_send(1, h).wait_recv()
        start_if(xh == 1, x_send, 4, 1, h)
        start_if(c == 1, c_send, 4, 2, h)

    def got_b(h):
        x_send(0, 1, h).wait_recv()
        c_send(3, 3, h).start()

    def got_c(k):
        for h in range(2):
            c_send(0, k, h).wait_recv()

    hg = 4 * z + 2 * xh + c
    scale = LOG2E / HS**0.5

    def bias(delta):
        return jnp.where(hg >= delta, 0.0, BIG).astype(F32)

    def attend(h, segs_of, first=False):
        rows = slice(h * ROWS, (h + 1) * ROWS)
        for j in range(2):
            segs = segs_of(j)
            keys = jnp.concatenate([ref[0, lo : lo + size, :] for ref, lo, size, _, _ in segs], 0)
            vals = jnp.concatenate([ref[1, lo : lo + size, :] for ref, lo, size, _, _ in segs], 0)
            vals = jnp.concatenate([vals, jnp.ones(vals.shape, BF)], 1)
            for g in range(4):
                every = lax.dot_general(qb[j, g, rows, :], keys, NT, preferred_element_type=F32)
                scores, tops, at = [], [], 0
                for _, _, size, mask, b in segs:
                    s = every[:, at : at + size]
                    at += size
                    if mask is not None:
                        t = lax.broadcasted_iota(jnp.int32, s.shape, 0) + h * ROWS
                        k = lax.broadcasted_iota(jnp.int32, s.shape, 1)
                        s = jnp.where(k <= t if mask == "upto" else k > t, s, -BIG)
                    m = jnp.max(s, axis=1, keepdims=True)
                    scores.append(s)
                    tops.append(m if b is None else m - b)
                top = functools.reduce(jnp.maximum, tops)
                if first:
                    new = jnp.broadcast_to(top, (ROWS, HS))
                else:
                    old = mx[j, g, rows, :]
                    new = jnp.maximum(old, top)
                probs = []
                for s, (_, _, _, _, b) in zip(scores, segs):
                    m = new[:, :1] if b is None else new[:, :1] + b
                    probs.append(jnp.exp2((s - m) * scale).astype(BF))
                total = jnp.dot(jnp.concatenate(probs, 1), vals, preferred_element_type=F32)
                if first:
                    acc[j, g, rows, :] = total
                else:
                    a = jnp.exp2((old - new) * scale)
                    acc[j, g, rows, :] = acc[j, g, rows, :] * jnp.concatenate([a, a], 1) + total
                mx[j, g, rows, :] = new

    def diagonal(j):
        last = (own.at[0], j * SH, SH, "upto", None)
        return [(own.at[0], 0, SH, None, None), last] if j else [last]

    def far(j):
        edge = (own.at[4], j * SH, SH, "after", bias(8))
        return [edge] if j else [edge, (own.at[4], SH, SH, None, bias(8))]

    def full(ref, delta):
        return (ref, 0, CH, None, bias(delta))

    odd = [jnp.where(c == 0, p, q) for p, q in ((3, 1), (1, 5), (7, 3), (5, 7))]

    yp, ym = lax.rem(y + 1, 4), lax.rem(y + 3, 4)

    def piece(t):
        _, lo, n = PIECES[t]
        return slice(2 * lo, 2 * (lo + n)), pl.ds(2 * lo, 2 * n)

    def a_send(k, t):
        b = ab.at[y, piece(t)[1], :]
        return remote(b, b, ss_a.at[k, t], rs_a.at[k, t], dev(z, xh, ym if k else yp, xl, c))

    def a_relay(k, t):
        _, lo, n = PIECES[t]
        b = ab.at[yp if k else ym, pl.ds(2 * lo + k * n, n), :]
        return remote(b, b, ss_r.at[k, t], rs_r.at[k, t], dev(z, xh, ym if k else yp, xl, c))

    def a_start(t):
        for k in range(2):
            a_send(k, t).start()

    def a_got(t):
        for k in range(2):
            a_send(k, t).wait_recv()
            a_relay(k, t).start()

    def a_all(t):
        for k in range(2):
            a_relay(k, t).wait_recv()

    def finish(h):
        attend(h, lambda j: [full(own.at[3], 6), full(oth.at[3], odd[3])])
        rows = slice(h * ROWS, (h + 1) * ROWS)
        for j in range(2):
            for g in range(4):
                a = acc[j, g, rows, :]
                a = (a[:, :HS] / a[:, HS:]).astype(BF)
                for p, lo, n in PIECES:
                    if p == h:
                        row, tok = 2 * lo + j * n, lo - h * ROWS
                        ab[y, row : row + n, g * HS : (g + 1) * HS] = a[tok : tok + n]

    def partial(t, side):
        total = None
        for yy in range(4):
            w = wb[yy // 2, pl.ds(side * 4, 4), :, :, (yy % 2) * CH : (yy % 2 + 1) * CH].reshape(CH, CH)
            u = lax.dot_general(ab[yy, piece(t)[0], :], w, NT, preferred_element_type=F32)
            total = u if total is None else total + u
        return total

    def p_send(t):
        rows = piece(t)[1]
        return remote(pa.at[rows, :], pr.at[rows, :], ss_p.at[t], rs_p.at[t], d_l)

    def p_away(t):
        a_all(t)
        pa[piece(t)[0], :] = partial(t, 1 - xl).astype(BF)
        p_send(t).start()

    def p_own(t):
        pf[piece(t)[0], :] = partial(t, xl)

    def o_send(t, j, i):
        _, lo, n = PIECES[t]
        source, place = rb.at[i, pl.ds(2 * lo + j * n, n), :], out.at[y, pl.ds(lo, n), :]
        return remote(source, place, ss_o.at[t, 2 * j + i], rs_o.at[y, t], dev(z, xh, 2 * c + j, xl, i))

    def o_here(j, i):
        return jnp.logical_and(y == 2 * c + j, c == i)

    def p_got(t):
        p_send(t).wait_recv()
        rows = piece(t)[0]
        _, lo, n = PIECES[t]
        for i in range(2):
            cols = slice(i * SH, (i + 1) * SH)
            rb[i, rows, :] = (pf[rows, cols] + pr[rows, cols].astype(F32)).astype(BF)
        for j in range(2):
            for i in range(2):
                @pl.when(o_here(j, i))
                def _():
                    out[y, lo : lo + n, :] = rb[i, 2 * lo + j * n : 2 * lo + (j + 1) * n, :]

                @pl.when(jnp.logical_not(o_here(j, i)))
                def _():
                    o_send(t, j, i).start()

    def near(j):
        return diagonal(j) + [full(own.at[2], 4), full(oth.at[0], odd[0])]

    def middle(j):
        return [full(own.at[1], 2), full(oth.at[1], odd[1]), full(oth.at[2], odd[2])] + far(j)

    got_z1(0)
    got_z1(1)
    w_ring(1, 0, 1).start()
    w_got(1, 0, 0)
    w_got(0, 0, 1)
    got_c(0)
    attend(0, near, first=True)
    w_got(0, 1, 0)
    got_a(0)
    got_z2(0)
    w_got(0, 1, 1)
    attend(1, near, first=True)
    got_a(1)
    got_z2(1)
    w_got(0, 2, 0)
    got_c(1)
    got_c(2)
    attend(0, middle)
    got_b(0)
    got_b(1)
    w_got(0, 2, 1)
    w_got(1, 0, 1)
    w_got(1, 1, 0)
    w_got(0, 3, 0)
    got_c(3)
    finish(0)
    a_start(0)
    a_start(1)
    attend(1, middle)
    w_got(1, 1, 1)
    w_got(0, 3, 1)
    finish(1)
    a_got(0)
    a_start(2)
    w_got(0, 4, 0)
    w_got(1, 2, 1)
    w_core(7, lax.rem(z + 5, 8)).start()
    a_got(1)
    a_start(3)
    for k in range(8):
        w_core(k, z).wait_recv()
    p_away(0)
    p_own(0)
    a_got(2)
    a_start(4)
    p_away(1)
    a_got(3)
    p_own(1)
    p_got(0)
    p_away(2)
    a_got(4)
    p_own(2)
    p_away(3)
    p_own(3)
    p_got(1)
    p_away(4)
    p_own(4)
    for t in range(2, 5):
        p_got(t)

    for yy in range(4):
        @pl.when(jnp.logical_not(jnp.logical_and(yy == y, c == y // 2)))
        def _():
            for t, (_, lo, n) in enumerate(PIECES):
                place = out.at[yy, pl.ds(lo, n), :]
                remote(rb.at[0, pl.ds(lo, n), :], place, ss_o.at[0, 0], rs_o.at[yy, t], d_c).wait_recv()
    for i in range(2):
        @pl.when(is_remote(i))
        def _():
            for copy in to_head(i):
                copy.wait_send()
    w_x.wait_send()
    for k, n, h in RING:
        w_ring(k, n, h).wait_send()
    for h in range(2):
        for k in range(2):
            z_send(k, h).wait_send()
            x_send(0, k, h).wait_send()
        for k in range(4):
            c_send(0, k, h).wait_send()
    for k in range(8):
        w_core(k, z).wait_send()
    for t in range(len(PIECES)):
        for k in range(2):
            a_send(k, t).wait_send()
            a_relay(k, t).wait_send()
        p_send(t).wait_send()
        for j in range(2):
            for i in range(2):
                @pl.when(jnp.logical_not(o_here(j, i)))
                def _():
                    o_send(t, j, i).wait_send()


def body(queries, keys, values, out_weight):
    tokens = queries.shape[0]
    q = queries.reshape(tokens, 2, 4, HS).transpose(1, 2, 0, 3)
    kv = jnp.stack([keys, values]).transpose(2, 0, 1, 3)
    dma = pltpu.SemaphoreType.DMA
    shapes = [(2,)] * 4 + [(2, 2)] * 4 + [(4, 2)] * 2 + [(1,)] * 2 + [(8, 2)] * 2 + [(8,)] * 2 + [(2, 5)] * 4 + [(5,)] * 2 + [(5, 4), (4, 5)]
    sems = [dma(shape) for shape in shapes]
    vmem = pl.BlockSpec(memory_space=pltpu.VMEM)
    r = pl.pallas_call(
        kernel,
        name="layer",
        out_shape=jax.ShapeDtypeStruct((4, SH, SH), BF),
        in_specs=[vmem] * 3,
        out_specs=vmem,
        scratch_shapes=[
            pltpu.VMEM((2, 4, SH, HS), BF),
            pltpu.VMEM((5, 2, CH, HS), BF),
            pltpu.VMEM((4, 2, CH, HS), BF),
            pltpu.VMEM((2, 8, 2, 64, 1024), BF),
            pltpu.VMEM((2, 4, SH, HS), F32),
            pltpu.VMEM((2, 4, SH, 2 * HS), F32),
            pltpu.VMEM((4, CH, CH), BF),
            pltpu.VMEM((CH, CH), F32),
            pltpu.VMEM((CH, CH), BF),
            pltpu.VMEM((CH, CH), BF),
            pltpu.VMEM((2, CH, SH), BF),
            *sems,
        ],
        compiler_params=pltpu.CompilerParams(
            collective_id=0, has_side_effects=True, vmem_limit_bytes=48 * 2**20
        ),
    )(q, kv, out_weight.T)
    return r.reshape(4, tokens, 4, 64).transpose(1, 2, 0, 3).reshape(tokens, 1024)


def solution(mesh):
    return jax.shard_map(
        body,
        mesh=mesh,
        in_specs=(
            P("seq", "head", None),
            P("seq", "head", None),
            P("seq", "head", None),
            P("head", "seq"),
        ),
        out_specs=P("seq", "head"),
        check_vma=False,
    )
```
